256 devices in a mesh: tm: 8 (over x, core), space: 32 (over z, y).
Axes of the slice: x: 4, y: 4, z: 8, core: 2. Of those that a mesh axis runs over, the one named last changes fastest.
Arguments:
- links: float32 [64, 3, 2, 3, 2, 110592], P('tm', None, None, None, None, 'space'), may hold values from -1 to 1, as said below
Outputs:
- new_links: float32 [64, 3, 2, 3, 2, 110592], P('tm', None, None, None, None, 'space')
- theta: float32 [], replicated
- deficit: float32 [64], P('tm')
The draws below stay inside these ranges and needn't reach their ends.
Inputs may be any that keep to these rules, and one draw needn't show every extreme that they name: `links`: each link's two stored rows are orthonormal complex 3-vectors, the first two rows of a special unitary matrix.
All inputs are finite; a program needn't handle non-finite values.
Results may differ from the reference program's by a relative error of at most 0.00013.
Values sent between devices are 32-bit elements; how exact they have to be, the bound alone decides.
No kernel may reach another device: no remote copies, remote signals or barrier semaphores. Data moves between devices by JAX's collectives and lax.ppermute only.
A program may use at most 128 MiB of HBM per device.

```python
import math
import jax
import jax.numpy as jnp
from jax import lax

EXTENT = 48
SLICES = 64


def draw_links(key, part):
    sites = EXTENT ** 3
    subkeys = jax.random.split(key, 1)
    site_index = jnp.arange(sites, dtype=jnp.int32)
    row_index = (site_index // EXTENT - 1) % (EXTENT * EXTENT)
    ycoord = (row_index // EXTENT).astype(jnp.float32)
    tcoord = jnp.arange(SLICES, dtype=jnp.float32)
    strength = 0.15 + 0.35 * (0.5 * tcoord[:, None] / SLICES + 0.5 * ycoord[None, :] / EXTENT)
    full_shape = (SLICES, 3, 2, 3, 2, sites)
    noise_field = jnp.clip(0.6 * jax.random.normal(subkeys[0], full_shape, jnp.float32), -1.0, 1.0)
    unit_rows = (jnp.arange(2)[:, None] == jnp.arange(3)[None, :]).astype(jnp.float32)
    unit_rows = unit_rows[:, :, None] * jnp.array([1.0, 0.0], jnp.float32)
    raw_rows = noise_field * strength[:, None, None, None, None, :] + unit_rows[None, None, :, :, :, None]
    vector_one = raw_rows[:, :, 0]
    vector_two = raw_rows[:, :, 1]
    length = jnp.sqrt(jnp.sum(vector_one * vector_one, axis=(2, 3)))
    row_one = vector_one / length[:, :, None, None, :]
    correlation_real = jnp.sum(row_one[:, :, :, 0] * vector_two[:, :, :, 0] + row_one[:, :, :, 1] * vector_two[:, :, :, 1], axis=2)
    correlation_imag = jnp.sum(row_one[:, :, :, 0] * vector_two[:, :, :, 1] - row_one[:, :, :, 1] * vector_two[:, :, :, 0], axis=2)
    rest_real = vector_two[:, :, :, 0] - (correlation_real[:, :, None] * row_one[:, :, :, 0] - correlation_imag[:, :, None] * row_one[:, :, :, 1])
    rest_imag = vector_two[:, :, :, 1] - (correlation_real[:, :, None] * row_one[:, :, :, 1] + correlation_imag[:, :, None] * row_one[:, :, :, 0])
    row_two = jnp.stack([rest_real, rest_imag], axis=3)
    length = jnp.sqrt(jnp.sum(row_two * row_two, axis=(2, 3)))
    row_two = row_two / length[:, :, None, None, :]
    return jnp.stack([row_one, row_two], axis=2).astype(jnp.float32)


def setup_inputs(seed: int = 0) -> dict:
    splits = jax.random.split(jax.random.key(seed), 2)
    links = draw_links(jax.random.fold_in(splits[1], 71), 0)
    return dict(links=links)


root_three = math.sqrt(3.0)
step_size = 0.08
top_momentum = 12.0
storage_offset = 1

def complex_mul(p, q):
    return (p[0] * q[0] - p[1] * q[1], p[0] * q[1] + p[1] * q[0])

def complex_add(p, q):
    return (p[0] + q[0], p[1] + q[1])

def complex_sub(p, q):
    return (p[0] - q[0], p[1] - q[1])

def complex_conj(p):
    return (p[0], -p[1])

def matrix_mul(left, right):
    rows_out = []
    for i in range(len(left)):
        entries = []
        for j in range(3):
            summed = complex_mul(left[i][0], right[0][j])
            for k in (1, 2):
                summed = complex_add(summed, complex_mul(left[i][k], right[k][j]))
            entries.append(summed)
        rows_out.append(entries)
    return rows_out

def dagger_of(matrix):
    return [[complex_conj(matrix[j][i]) for j in range(3)] for i in range(3)]

def cross_conj(row_one, row_two):
    row_three = []
    for k in range(3):
        a = complex_mul(row_one[(k + 1) % 3], row_two[(k + 2) % 3])
        b = complex_mul(row_one[(k + 2) % 3], row_two[(k + 1) % 3])
        row_three.append(complex_conj(complex_sub(a, b)))
    return row_three

def full_matrix(entry_of):
    row_one = [(entry_of(0, c, 0), entry_of(0, c, 1)) for c in range(3)]
    row_two = [(entry_of(1, c, 0), entry_of(1, c, 1)) for c in range(3)]
    return [row_one, row_two, cross_conj(row_one, row_two)]

def gradient_of(current, behind):
    gradient = []
    for i in range(3):
        entries = []
        for j in range(3):
            summed = complex_sub(behind[0][i][j], current[0][i][j])
            for d in (1, 2):
                summed = complex_add(summed, complex_sub(behind[d][i][j], current[d][i][j]))
            entries.append(summed)
        gradient.append(entries)
    return gradient

def algebra_of(gradient):
    g = gradient
    return [g[0][1][1] + g[1][0][1], g[0][1][0] - g[1][0][0], g[0][0][1] - g[1][1][1], g[0][2][1] + g[2][0][1], g[0][2][0] - g[2][0][0], g[1][2][1] + g[2][1][1], g[1][2][0] - g[2][1][0], (g[0][0][1] + g[1][1][1] - 2.0 * g[2][2][1]) / root_three]

def rotation_of(algebra):
    half_step = 0.5 * step_size
    zeros_like = jnp.zeros_like(algebra[0])
    diag_zero = algebra[2] + algebra[7] / root_three
    diag_one = -algebra[2] + algebra[7] / root_three
    diag_two = -2.0 * algebra[7] / root_three
    hermitian = [[(diag_zero, zeros_like), (algebra[0], -algebra[1]), (algebra[3], -algebra[4])], [(algebra[0], algebra[1]), (diag_one, zeros_like), (algebra[5], -algebra[6])], [(algebra[3], algebra[4]), (algebra[5], algebra[6]), (diag_two, zeros_like)]]
    generator = [[(-half_step * h[1], half_step * h[0]) for h in row] for row in hermitian]
    square = matrix_mul(generator[:2], generator)
    rows_two = []
    for i in range(2):
        entries = []
        for j in range(3):
            real_value = generator[i][j][0] + 0.5 * square[i][j][0]
            if i == j:
                real_value = real_value + 1.0
            entries.append((real_value, generator[i][j][1] + 0.5 * square[i][j][1]))
        rows_two.append(entries)
    length = jnp.sqrt(sum((p[0] * p[0] + p[1] * p[1] for p in rows_two[0])))
    row_one = [(p[0] / length, p[1] / length) for p in rows_two[0]]
    correlation = complex_mul(complex_conj(row_one[0]), rows_two[1][0])
    for k in (1, 2):
        correlation = complex_add(correlation, complex_mul(complex_conj(row_one[k]), rows_two[1][k]))
    row_two = [complex_sub(rows_two[1][k], complex_mul(correlation, row_one[k])) for k in range(3)]
    length = jnp.sqrt(sum((p[0] * p[0] + p[1] * p[1] for p in row_two)))
    row_two = [(p[0] / length, p[1] / length) for p in row_two]
    return [row_one, row_two, cross_conj(row_one, row_two)]

def two_rows(product, axis):
    return jnp.stack([jnp.stack([jnp.stack(product[r][c], axis=axis) for c in range(3)], axis=axis) for r in range(2)], axis=axis)

def reference(links):
    extent = EXTENT
    slice_count = links.shape[0]
    wave_number = jnp.arange(extent, dtype=jnp.int32)
    wave_term = 4.0 * jnp.sin(math.pi * wave_number.astype(jnp.float32) / extent) ** 2
    momentum = wave_term[:, None, None] + wave_term[None, :, None] + wave_term[None, None, :]
    zero_mode = wave_number[:, None, None] + wave_number[None, :, None] + wave_number[None, None, :] == 0
    factor = jnp.where(zero_mode, 0.0, top_momentum / jnp.where(zero_mode, 1.0, momentum))
    roll_axes = (-1, -3, -2)

    def one_slice(slice_links):
        ordered = jnp.roll(slice_links, -storage_offset * extent, axis=-1)
        lattice = ordered.reshape(3, 2, 3, 2, extent, extent, extent)
        current = []
        behind = []
        for d in range(3):
            here = lattice[d]
            moved = jnp.roll(here, 1, axis=roll_axes[d])
            current.append(full_matrix(lambda r, c, p, arr=here: arr[r, c, p]))
            behind.append(full_matrix(lambda r, c, p, arr=moved: arr[r, c, p]))
        algebra = algebra_of(gradient_of(current, behind))
        theta_part = sum((jnp.sum(a * a) for a in algebra))
        spectrum = jnp.fft.fftn(jnp.stack(algebra), axes=(1, 2, 3))
        smooth = jnp.real(jnp.fft.ifftn(spectrum * factor, axes=(1, 2, 3))).astype(jnp.float32)
        rotation = rotation_of([smooth[a] for a in range(8)])
        new_dirs = []
        deficit_part = jnp.zeros((), jnp.float32)
        for d in range(3):
            ahead_rot = jax.tree.map(lambda a, ax=roll_axes[d]: jnp.roll(a, -1, axis=ax), rotation)
            product = matrix_mul(matrix_mul(rotation, current[d]), dagger_of(ahead_rot))
            deficit_part = deficit_part + jnp.sum(3.0 - product[0][0][0] - product[1][1][0] - product[2][2][0])
            new_dirs.append(two_rows(product, 0))
        result = jnp.stack(new_dirs).reshape(3, 2, 3, 2, extent ** 3)
        return (jnp.roll(result, storage_offset * extent, axis=-1), theta_part, deficit_part)
    new_links, thetas, deficits = lax.map(one_slice, links)
    theta = jnp.sum(thetas) / (slice_count * extent ** 3)
    deficit = deficits / extent ** 3
    return (new_links, theta, deficit)
```

```python
import functools
import math

import jax
import jax.numpy as jnp
import numpy as np
from jax import lax
from jax.experimental import pallas as pl
from jax.experimental.pallas import tpu as pltpu
from jax.sharding import Mesh
from jax.sharding import PartitionSpec as P

EXTENT = 48
SPACE = ("space_0", "space_1")
TM = ("tm_0", "tm_1")
TM_SPACE = ("tm_0", "tm_1", "space_0", "space_1")
SLICES = 8
ROWS = 72
SITES = ROWS * EXTENT
PLANE = EXTENT * EXTENT
WIDE = SITES + PLANE
GROUP = 7 * PLANE

root_three = math.sqrt(3.0)
step_size = 0.08
f32 = jnp.float32
bf16 = jnp.bfloat16


def from_behind(block, axis, distance):
    n = lax.axis_size(axis)
    return lax.ppermute(block, axis, [((i - distance) % n, i) for i in range(n)])


def basis():
    k = np.arange(25)[:, None]
    x = np.arange(EXTENT)[None, :]
    cos = np.cos(2 * np.pi * k * x / EXTENT) * math.sqrt(2 / EXTENT)
    cos[0] /= math.sqrt(2)
    cos[24] /= math.sqrt(2)
    sin = np.sin(2 * np.pi * k * x / EXTENT) * math.sqrt(2 / EXTENT)
    return np.concatenate([cos, sin[1:24]], axis=0)


def wave_terms():
    k = np.concatenate([np.arange(25), np.arange(1, 24)])
    return 4 * np.sin(np.pi * k / EXTENT) ** 2


def split_bf16(a):
    a = np.asarray(a, np.float32)
    hi = np.asarray(jnp.asarray(a).astype(bf16).astype(f32)) if False else a.astype(jnp.bfloat16)
    lo = (a - hi.astype(np.float32)).astype(jnp.bfloat16)
    return hi, lo


Q = basis()
P2 = wave_terms()
WX = np.einsum("kx,zw->kzwx", Q, np.eye(8)).reshape(384, 384)
WX_HI, WX_LO = split_bf16(WX)
Q_HI, Q_LO = split_bf16(Q)
QT_HI, QT_LO = split_bf16(Q.T)
Q_STACK = np.concatenate([Q_HI, Q_HI, Q_LO], axis=1)
QT_STACK = np.concatenate([QT_HI, QT_HI, QT_LO], axis=1)
PZ = np.repeat(P2[:, None], 128, axis=1).astype(np.float32)
PX = P2.astype(np.float32)
PXM = np.repeat(np.repeat(P2.reshape(6, 1, 8), 6, axis=1).reshape(36, 8), 16, axis=1)
PZM = np.repeat(np.tile(P2.reshape(6, 8).T[:, None, :], (1, 6, 1)).reshape(8, 36, 1), 128, axis=2)
PSUM = (PXM[None] + PZM).astype(np.float32)


def zero_green(distance):
    d = np.arange(EXTENT)
    mean = np.mean(d * d / 96 - d / 2)
    return float(12 * (distance * distance / 96 - distance / 2 - mean))


def cmul(p, q):
    return (p[0] * q[0] - p[1] * q[1], p[0] * q[1] + p[1] * q[0])


def cmul_conj(p, q):
    return (p[0] * q[0] + p[1] * q[1], p[1] * q[0] - p[0] * q[1])


def cadd(p, q):
    return (p[0] + q[0], p[1] + q[1])


def csub(p, q):
    return (p[0] - q[0], p[1] - q[1])


def cross_conj(a, b):
    out = []
    for k in range(3):
        p = cmul(a[(k + 1) % 3], b[(k + 2) % 3])
        q = cmul(a[(k + 2) % 3], b[(k + 1) % 3])
        out.append((p[0] - q[0], q[1] - p[1]))
    return out


def algebra_of(u0, u1):
    u2 = cross_conj(u0, u1)
    return [
        u0[1][1] + u1[0][1],
        u0[1][0] - u1[0][0],
        u0[0][1] - u1[1][1],
        u0[2][1] + u2[0][1],
        u0[2][0] - u2[0][0],
        u1[2][1] + u2[1][1],
        u1[2][0] - u2[1][0],
        (u0[0][1] + u1[1][1] - 2.0 * u2[2][1]) * (1.0 / root_three),
    ]


def rotation_of(a):
    half = 0.5 * step_size
    a = [half * v for v in a]
    e = a[7] * (1.0 / root_three)
    diag = [a[2] + e, e - a[2], -2.0 * e]
    zero = jnp.zeros_like(a[0])
    x = [
        [(zero, diag[0]), (a[1], a[0]), (a[4], a[3])],
        [(-a[1], a[0]), (zero, diag[1]), (a[6], a[5])],
        [(-a[4], a[3]), (-a[6], a[5]), (zero, diag[2])],
    ]

    def entry(i, j):
        total = None
        for k in range(3):
            p, q = x[i][k], x[k][j]
            if i == k and k == j:
                term = (-p[1] * q[1], None)
            elif i == k:
                term = (-p[1] * q[1], p[1] * q[0])
            elif k == j:
                term = (-p[1] * q[1], p[0] * q[1])
            else:
                term = cmul(p, q)
            if total is None:
                total = term
            else:
                re = total[0] + term[0]
                if total[1] is None:
                    im = term[1]
                elif term[1] is None:
                    im = total[1]
                else:
                    im = total[1] + term[1]
                total = (re, im)
        re = 0.5 * total[0] + x[i][j][0] if i != j else 0.5 * total[0] + 1.0
        im = 0.5 * total[1] + x[i][j][1]
        return (re, im)

    m0 = [entry(0, j) for j in range(3)]
    m1 = [entry(1, j) for j in range(3)]
    inv = lax.rsqrt(sum(p[0] * p[0] + p[1] * p[1] for p in m0))
    r0 = [(p[0] * inv, p[1] * inv) for p in m0]
    corr = cmul_conj(m1[0], r0[0])
    for k in (1, 2):
        corr = cadd(corr, cmul_conj(m1[k], r0[k]))
    w = [csub(m1[k], cmul(corr, r0[k])) for k in range(3)]
    inv = lax.rsqrt(sum(p[0] * p[0] + p[1] * p[1] for p in w))
    r1 = [(p[0] * inv, p[1] * inv) for p in w]
    return r0, r1


def two_rows_of(load):
    u0 = [(load(2 * c), load(2 * c + 1)) for c in range(3)]
    u1 = [(load(6 + 2 * c), load(6 + 2 * c + 1)) for c in range(3)]
    return u0, u1


def gradient_kernel(idx, links, beyond, out, hs, hz24, zb):
    yc = idx[1]
    even = (yc % 2) == 0

    def project(q, carry):
        off = pl.multiple_of(q * 384, 128)
        for d in range(3):
            u0, u1 = two_rows_of(lambda n: links[12 * d + n, :, pl.ds(off, 384)])
            for c, h in enumerate(algebra_of(u0, u1)):
                hs[d * 8 + c, :, pl.ds(off, 384)] = h
        return carry

    lax.fori_loop(0, 9, project, 0)
    for d in range(3):
        u0, u1 = two_rows_of(lambda n: beyond[12 * d + n])
        for c, h in enumerate(algebra_of(u0, u1)):
            hs[d * 8 + c, :, SITES : SITES + 128] = h
    u0, u1 = two_rows_of(lambda n: beyond[36 + n])
    for c, h in enumerate(algebra_of(u0, u1)):
        hz24[c] = h

    width = SITES + 128
    xzero = (lax.broadcasted_iota(jnp.int32, (8, width), 1) % EXTENT) == 0
    lane = lax.broadcasted_iota(jnp.int32, (8, 128), 1)
    second = (lane >= 48) & (lane < 96)

    def combine(c, carry):
        hx = hs[c]
        hy = hs[8 + c]
        hz = hs[16 + c]
        zb[...] = pltpu.roll(hz, 48, 1)
        fix_a = pltpu.roll(hz[:, 2304:2432], 48, 1)
        fix_b = pltpu.roll(hz24[c], 48, 1)
        fix_c = pltpu.roll(hz[:, 3456:3584], 48, 1)
        sel_even = second & even
        sel_odd = second & jnp.logical_not(even)
        zb[:, 0:128] = jnp.where(sel_even, fix_a, zb[:, 0:128])
        zb[:, 2304:2432] = jnp.where(sel_even, fix_b, zb[:, 2304:2432])
        zb[:, 1152:1280] = jnp.where(sel_odd, fix_c, zb[:, 1152:1280])
        bx = jnp.where(xzero, pltpu.roll(hx, width - 47, 1), pltpu.roll(hx, 1, 1))
        p = (bx - hx) + (zb[...] - hz) - hy
        p = pltpu.roll(p, width - 48, 1)
        ha = pltpu.roll(hy, width - 48, 1)
        k = lax.rem(c // 2 - yc + 4, 4)
        f = c % 2
        out[k, f, :, 0:PLANE] = p[:, 0:PLANE]
        out[k, f, :, PLANE:SITES] = p[:, PLANE:SITES] + ha[:, 0 : SITES - PLANE]
        out[k, f, :, SITES:WIDE] = ha[:, SITES - PLANE : SITES]
        return carry

    lax.fori_loop(0, 8, combine, 0)


def lambda_of(m):
    s = jnp.sqrt(m + 0.25 * m * m)
    return 1.0 / (1.0 + 0.5 * m + s), s


def split_value(a):
    hi = a.astype(bf16)
    return hi, (a - hi.astype(f32)).astype(bf16)


def dot(a, b, ca, cb):
    return lax.dot_general(a, b, (((ca,), (cb,)), ((), ())), preferred_element_type=f32)


def stack_of(a):
    hi, lo = split_value(a)
    return jnp.concatenate([hi, lo, hi], axis=0)


def forward_kernel(
    idx, px, r0, r1, r2, r3, wxh, wxl, qs, pz, sout, own, first, last, theta, gs, ds, es
):
    yc = idx[1]
    gs[...] = jnp.zeros((2, 8, GROUP), f32)
    for k, r in enumerate((r0, r1, r2, r3)):
        off = pl.multiple_of(lax.rem(yc - k + 4, 4) * SITES, 128)
        gs[:, :, pl.ds(off, WIDE)] += r[...]
    first[...] = gs[:, :, 0:PLANE]
    last[...] = gs[:, :, 6 * PLANE : 7 * PLANE]
    mid = gs[:, :, PLANE : 6 * PLANE]
    theta[...] = jnp.sum((mid * mid).reshape(2, 8, 5 * PLANE // 128, 128), axis=(0, 2)) if False else sum(
        gs[f, :, 128 * n : 128 * n + 128] ** 2 for f in range(2) for n in range(18, 108)
    )

    zeros = jnp.zeros((16, 384), f32)

    def along_x(j, carry):
        pieces = []
        for y in range(7):
            for f in range(2):
                pieces.append(gs[f, :, pl.ds(pl.multiple_of(PLANE * y + 384 * j, 128), 384)])
        b = jnp.concatenate(pieces + [zeros], axis=0)
        bh, bl = split_value(b)
        wh = wxh[...]
        out = dot(wh, bh, 1, 1) + dot(wh, bl, 1, 1) + dot(wxl[...], bh, 1, 1)
        ds[:, pl.ds(pl.multiple_of(8 * j, 8), 8), :] = out.reshape(EXTENT, 8, 128)
        return carry

    lax.fori_loop(0, 6, along_x, 0)

    gi = lax.broadcasted_iota(jnp.int32, (EXTENT, 128), 1) // 16

    def along_z(m, carry):
        accp = jnp.zeros((EXTENT, 128), f32)
        accm = jnp.zeros((EXTENT, 128), f32)
        for g in range(8):
            k = m * 8 + g
            e = dot(qs[...], stack_of(ds[k]), 1, 0)
            if g == 0:
                es[m] = e[0:8]
            lam, s = lambda_of(px[k] + pz[...])
            lam2 = lam * lam
            lam4 = lam2 * lam2
            up = e + jnp.where(gi >= 1, lam, 0.0) * pltpu.roll(e, 16, 1)
            up = up + jnp.where(gi >= 2, lam2, 0.0) * pltpu.roll(up, 32, 1)
            up = up + jnp.where(gi >= 4, lam4, 0.0) * pltpu.roll(up, 64, 1)
            down = e + jnp.where(gi <= 6, lam, 0.0) * pltpu.roll(e, 112, 1)
            down = down + jnp.where(gi <= 5, lam2, 0.0) * pltpu.roll(down, 96, 1)
            down = down + jnp.where(gi <= 3, lam4, 0.0) * pltpu.roll(down, 64, 1)
            own[k] = (6.0 / s) * (up + down - e)
            accp = jnp.where(gi == g, pltpu.roll(up, ((g - 6) * 16) % 128, 1), accp)
            accm = jnp.where(gi == g, pltpu.roll(down, (g * 16) % 128, 1), accm)
        for i in range(6):
            sout[pl.ds(m * 6 + i, 8, stride=72), :] = accp[8 * i : 8 * i + 8]
            sout[pl.ds(36 + m * 6 + i, 8, stride=72), :] = accm[8 * i : 8 * i + 8]
        return carry

    lax.fori_loop(0, 6, along_z, 0)

    e0 = es[0]
    gt = lax.broadcasted_iota(jnp.int32, (8, 128), 1) // 16
    row = lax.broadcasted_iota(jnp.int32, (8, 128), 0)
    total = zero_green(0) * e0
    for n in range(1, 8):
        weight = jnp.where(gt >= n, zero_green(n), zero_green(8 - n))
        total = total + weight * pltpu.roll(e0, 16 * n, 1)
    own[0, 0:8, :] = jnp.where(row == 0, total, own[0, 0:8, :])
    yf = gt.astype(f32)

    def over_groups(v):
        for n in (16, 32, 64):
            v = v + pltpu.roll(v, n, 1)
        return v

    m1 = over_groups(yf * e0)
    m2 = over_groups(yf * yf * e0)
    here = (row == 0) & (gt == 0)
    sout[0:8, :] = jnp.where(here, m1, sout[0:8, :])
    sout[36:44, :] = jnp.where(here, pltpu.roll(m2, 0, 0), sout[36:44, :])


def solve_kernel(idx, s, psum, out):
    zc = idx[0]
    lam, root = lambda_of(psum[zc])
    lam2 = lam * lam
    lam6 = lam2 * lam2 * lam2
    lam12 = lam6 * lam6
    lam24 = lam12 * lam12
    row = lax.broadcasted_iota(jnp.int32, (36, 128), 0)
    lane = lax.broadcasted_iota(jnp.int32, (36, 128), 1)
    zero = (row == 0) & (lane < 16) & (zc == 0)
    kappa = 6.0 / root / (1.0 - lam24 * lam24)
    coef = []
    power = jnp.ones_like(lam)
    for k in range(1, 9):
        coef.append(kappa * power)
        power = power * lam6
    plus = [s[72 * n : 72 * n + 36, :] for n in range(8)]
    minus = [s[72 * n + 36 : 72 * n + 72, :] for n in range(8)]
    total_p = sum(plus)
    total_m = sum(minus)
    coef_a = [jnp.where(zero, 12.0 * (0.5 - k / 8.0) if k < 8 else 0.0, coef[k - 1]) for k in range(1, 9)]
    for t in range(8):
        a = coef_a[0] * plus[(t - 1) % 8]
        b = coef[0] * minus[(t + 1) % 8]
        for k in range(2, 9):
            a = a + coef_a[k - 1] * plus[(t - k) % 8]
            b = b + coef[k - 1] * minus[(t + k) % 8]
        a = a + jnp.where(zero, 0.125 * (total_m - minus[t]), 0.0)
        b = jnp.where(zero, -0.25 * (total_p - plus[t]), b)
        out[72 * t : 72 * t + 36, :] = a
        out[72 * t + 36 : 72 * t + 72, :] = b


def spread_groups(v, gi):
    level = [v]
    for width in (4, 2, 1):
        bit = (gi // width) % 2
        out = []
        for a in level:
            if width == 4:
                rolled = pltpu.roll(a, 64, 1)
            else:
                up = pltpu.roll(a, 16 * width, 1)
                down = pltpu.roll(a, 128 - 16 * width, 1)
                rolled = jnp.where(bit == 0, down, up)
            out.append(jnp.where(bit == 0, a, rolled))
            out.append(jnp.where(bit == 0, rolled, a))
        level = out
    return level


def backward_kernel(idx, px, ab, own, wxh, wxl, qts, pz, first, before, theta_in, out, theta, ds, gs):
    yc = idx[1]
    acc = theta_in[...]
    for f in range(2):
        for n in range(18):
            v = first[f, :, 128 * n : 128 * n + 128] + before[f, :, 128 * n : 128 * n + 128]
            acc = acc + v * v
    theta[...] = acc

    gi = lax.broadcasted_iota(jnp.int32, (EXTENT, 128), 1) // 16
    row = lax.broadcasted_iota(jnp.int32, (EXTENT, 128), 0)
    gr = 6 - gi
    gif = gi.astype(f32)

    def along_z(m, carry):
        ta = jnp.concatenate([ab[pl.ds(m * 6 + i, 8, stride=72), :] for i in range(6)], axis=0)
        tb = jnp.concatenate([ab[pl.ds(36 + m * 6 + i, 8, stride=72), :] for i in range(6)], axis=0)
        las = spread_groups(ta, gi)
        lbs = spread_groups(tb, gi)
        for g in range(8):
            k = m * 8 + g
            lam, _ = lambda_of(px[k] + pz[...])
            lam2 = lam * lam
            lam4 = lam2 * lam2
            wa = jnp.where(gi % 2 == 1, lam, 1.0) * jnp.where((gi // 2) % 2 == 1, lam2, 1.0)
            wa = wa * jnp.where(gi >= 4, lam4, 1.0)
            wb = jnp.where(gr % 2 == 1, lam, 1.0) * jnp.where((gr // 2) % 2 == 1, lam2, 1.0)
            wb = wb * jnp.where(gr >= 4, lam4, 1.0)
            if g == 0:
                wb = jnp.where((row == 0) & (m == 0), gif, wb)
            u = own[k] + las[g] * wa + lbs[g] * wb
            ds[k] = dot(qts[...], stack_of(u), 1, 0)
        return carry

    lax.fori_loop(0, 6, along_z, 0)

    def along_x(j, carry):
        d = ds[:, pl.ds(pl.multiple_of(8 * j, 8), 8), :].reshape(384, 128)
        dt = jnp.transpose(d)
        dh, dl = split_value(dt)
        wh = wxh[...]
        o = dot(dh, wh, 1, 0) + dot(dl, wh, 1, 0) + dot(dh, wxl[...], 1, 0)
        for y in range(7):
            for f in range(2):
                gs[f, :, pl.ds(pl.multiple_of(PLANE * y + 384 * j, 128), 384)] = o[16 * y + 8 * f : 16 * y + 8 * f + 8]
        return carry

    lax.fori_loop(0, 6, along_x, 0)
    for k in range(4):
        off = pl.multiple_of(lax.rem(yc + k, 4) * SITES, 128)
        out[k] = gs[:, :, pl.ds(off, WIDE)]


def rotate_kernel(idx, r0, r1, r2, r3, rows, links, out, deficit, sm, gs, fix):
    yc = idx[1]
    even = (yc % 2) == 0
    lane = lax.broadcasted_iota(jnp.int32, (8, 128), 1)
    for k, r in enumerate((r0, r1, r2, r3)):
        c0 = 2 * lax.rem(yc - k + 4, 4)
        for f in range(2):
            sm[c0 + f] = pltpu.roll(r[f], 48, 1)
    for c in range(8):
        sm[c, :, 0:128] = jnp.where(lane < 48, rows[c], sm[c, :, 0:128])

    def store_rotation(load, store):
        g0, g1 = rotation_of([load(c) for c in range(8)])
        g2 = cross_conj(g0, g1)
        for i, g in enumerate((g0, g1, g2)):
            for c in range(3):
                for p in range(2):
                    store(6 * i + 2 * c + p, g[c][p])

    def rotations(q, carry):
        off = pl.multiple_of(q * 384, 128)

        def store(n, v):
            gs[n, :, pl.ds(off, 384)] = v

        store_rotation(lambda c: sm[c, :, pl.ds(off, 384)], store)
        return carry

    lax.fori_loop(0, 15, rotations, 0)

    def store_fix(n, v):
        fix[0, n] = v

    store_rotation(lambda c: pltpu.roll(rows[c], 80, 1), store_fix)
    for n in range(18):
        fix[1, n] = pltpu.roll(gs[n, :, 0:128], 80, 1)
    deficit[...] = jnp.zeros((8, 128), f32)
    xlast = (lax.broadcasted_iota(jnp.int32, (8, 384), 1) % EXTENT) == EXTENT - 1

    def products(q, carry):
        off = pl.multiple_of(q * 384, 128)
        far = pl.multiple_of(q * 384 + PLANE, 128)
        from_fix = ((q == 0) & even) | ((q == 3) & jnp.logical_not(even)) | ((q == 6) & even)
        which = jnp.where(q == 6, 1, 0)
        head = (lane < 48) & from_fix

        def here(n):
            return gs[n, :, pl.ds(off, 384)]

        def ahead_x(n):
            v = here(n)
            return jnp.where(xlast, pltpu.roll(v, 47, 1), pltpu.roll(v, 383, 1))

        def ahead_y(n):
            return gs[n, :, pl.ds(far, 384)]

        def ahead_z(n):
            v = pltpu.roll(gs[n, :, pl.ds(off, 512)], 512 - 48, 1)[:, 0:384]
            return jnp.concatenate([jnp.where(head, fix[which, n], v[:, 0:128]), v[:, 128:384]], axis=1)

        def matrix(load):
            return [[(load(6 * i + 2 * c), load(6 * i + 2 * c + 1)) for c in range(3)] for i in range(3)]

        g = matrix(here)
        acc = jnp.zeros((8, 384), f32)
        for d, ahead in enumerate((ahead_x, ahead_y, ahead_z)):
            u0, u1 = two_rows_of(lambda n: links[12 * d + n, :, pl.ds(off, 384)])
            u = [u0, u1, cross_conj(u0, u1)]
            h = matrix(ahead)
            rows_out = []
            for i in range(2):
                t = []
                for j in range(3):
                    v = cmul(g[i][0], u[0][j])
                    for k in (1, 2):
                        v = cadd(v, cmul(g[i][k], u[k][j]))
                    t.append(v)
                line = []
                for j in range(3):
                    v = cmul_conj(t[0], h[j][0])
                    for k in (1, 2):
                        v = cadd(v, cmul_conj(t[k], h[j][k]))
                    line.append(v)
                    out[12 * d + 6 * i + 2 * j, :, pl.ds(off, 384)] = v[0]
                    out[12 * d + 6 * i + 2 * j + 1, :, pl.ds(off, 384)] = v[1]
                rows_out.append(line)
            a, b = rows_out
            corner = (a[0][0] * b[1][0] - a[0][1] * b[1][1]) - (a[1][0] * b[0][0] - a[1][1] * b[0][1])
            acc = acc + (3.0 - a[0][0] - b[1][0] - corner)
        deficit[...] += acc[:, 0:128] + acc[:, 128:256] + acc[:, 256:384]
        return carry

    lax.fori_loop(0, 9, products, 0)


def shape(*dims):
    return jax.ShapeDtypeStruct(dims, f32)


def call(kernel, outs, scalars, scratch=()):
    def run(*args):
        vm = pl.BlockSpec(memory_space=pltpu.VMEM)
        sm = pl.BlockSpec(memory_space=pltpu.SMEM)
        return pl.pallas_call(
            kernel,
            in_specs=[sm] * scalars + [vm] * (len(args) - scalars),
            out_specs=[vm] * len(outs),
            out_shape=list(outs),
            scratch_shapes=list(scratch),
            compiler_params=pltpu.CompilerParams(vmem_limit_bytes=56 * 1024 * 1024),
        )(*args)

    return run


def exchange_y(pieces):
    return [pieces[0]] + [from_behind(pieces[k], "space_1", k) for k in (1, 2, 3)]


def exchange_z(a):
    return lax.all_to_all(a, "space_0", split_axis=0, concat_axis=0, tiled=True)


def body(links):
    zc = lax.axis_index("space_0")
    yc = lax.axis_index("space_1")
    idx = jnp.stack([zc, yc]).astype(jnp.int32)
    px = jnp.asarray(PX)
    flat = links.transpose(1, 2, 3, 4, 0, 5).reshape(36, SLICES, SITES)
    edge = jnp.concatenate([flat[:, :, 0:128], flat[24:36, :, 1152:1280]], axis=0)
    beyond = from_behind(edge, SPACE, -1)
    (pieces,) = call(
        gradient_kernel,
        [shape(4, 2, 8, WIDE)],
        1,
        [pltpu.VMEM((24, 8, SITES + 128), f32), pltpu.VMEM((8, 8, 128), f32), pltpu.VMEM((8, SITES + 128), f32)],
    )(idx, flat, beyond)
    r = exchange_y([pieces[k] for k in range(4)])
    moments, own, first, last, theta_mid = call(
        forward_kernel,
        [shape(576, 128), shape(48, 48, 128), shape(2, 8, PLANE), shape(2, 8, PLANE), shape(8, 128)],
        2,
        [pltpu.VMEM((2, 8, GROUP), f32), pltpu.VMEM((48, 48, 128), f32), pltpu.VMEM((6, 8, 128), f32)],
    )(idx, px, *r, jnp.asarray(WX_HI), jnp.asarray(WX_LO), jnp.asarray(Q_STACK), jnp.asarray(PZ))
    before = from_behind(last, "space_0", 1)
    moments = exchange_z(moments)
    (amps,) = call(solve_kernel, [shape(576, 128)], 1)(idx, moments, jnp.asarray(PSUM))
    amps = exchange_z(amps)
    windows, theta_part = call(
        backward_kernel,
        [shape(4, 2, 8, WIDE), shape(8, 128)],
        2,
        [pltpu.VMEM((48, 48, 128), f32), pltpu.VMEM((2, 8, GROUP), f32)],
    )(
        idx, px, amps, own, jnp.asarray(WX_HI), jnp.asarray(WX_LO), jnp.asarray(QT_STACK), jnp.asarray(PZ),
        first, before, theta_mid,
    )
    r = exchange_y([windows[k] for k in range(4)])

    def pick(a, start):
        return lax.slice_in_dim(a, start * 48, start * 48 + 48, axis=2)

    parity = (yc % 2) == 0
    small = []
    for a in r:
        extra = jnp.where(parity, pick(a, 48), pick(a, 24))
        small.append(jnp.concatenate([pick(a, 71), extra, jnp.zeros((2, 8, 32), f32)], axis=2))
    own_rows = jnp.stack(small)
    order = (yc - jnp.arange(4)) % 4
    own_rows = jnp.concatenate([lax.dynamic_slice_in_dim(own_rows, (yc - c) % 4, 1, axis=0) for c in range(4)], axis=0)
    rows = from_behind(own_rows.reshape(8, 8, 128), SPACE, 1)
    new_flat, deficit_part = call(
        rotate_kernel,
        [shape(36, 8, SITES), shape(8, 128)],
        1,
        [pltpu.VMEM((8, 8, WIDE), f32), pltpu.VMEM((18, 8, WIDE), f32), pltpu.VMEM((2, 18, 8, 128), f32)],
    )(idx, *r, rows, flat)
    new_links = new_flat.reshape(3, 2, 3, 2, SLICES, SITES).transpose(4, 0, 1, 2, 3, 5)

    theta_part = jnp.sum(theta_part)
    theta_tm = lax.psum(lax.psum(theta_part, "tm_1"), "tm_0")
    both = jnp.concatenate([jnp.sum(deficit_part, axis=1), theta_tm[None]])
    both = lax.psum(lax.psum(both, "space_1"), "space_0")
    theta = both[8] / (SLICES * 8 * EXTENT**3)
    deficit = both[:8] / EXTENT**3
    return (new_links, theta, deficit)


def solution(mesh):
    torus = Mesh(mesh.devices.reshape(4, 2, 8, 4), ("tm_0", "tm_1", "space_0", "space_1"))
    in_specs = (P(TM, None, None, None, None, SPACE),)
    out_specs = (P(TM, None, None, None, None, SPACE), P(), P(TM))
    return jax.shard_map(body, mesh=torus, in_specs=in_specs, out_specs=out_specs, check_vma=False)
```

```python
import functools
import math

import jax
import jax.numpy as jnp
import numpy as np
from jax import lax
from jax.experimental import pallas as pl
from jax.experimental.pallas import tpu as pltpu
from jax.sharding import Mesh
from jax.sharding import PartitionSpec as P

EXTENT = 48
SPACE = ("space_0", "space_1")
TM = ("tm_0", "tm_1")
TM_SPACE = ("tm_0", "tm_1", "space_0", "space_1")
SLICES = 8
ROWS = 72
SITES = ROWS * EXTENT
PLANE = EXTENT * EXTENT
WIDE = SITES + PLANE
WINDOW = WIDE + 128
GROUP = 8 * PLANE

root_three = math.sqrt(3.0)
step_size = 0.08
f32 = jnp.float32
bf16 = jnp.bfloat16


def from_behind(block, axis, distance):
    n = lax.axis_size(axis)
    return lax.ppermute(block, axis, [((i - distance) % n, i) for i in range(n)])


def basis():
    k = np.arange(25)[:, None]
    x = np.arange(EXTENT)[None, :]
    cos = np.cos(2 * np.pi * k * x / EXTENT) * math.sqrt(2 / EXTENT)
    cos[0] /= math.sqrt(2)
    cos[24] /= math.sqrt(2)
    sin = np.sin(2 * np.pi * k * x / EXTENT) * math.sqrt(2 / EXTENT)
    return np.concatenate([cos, sin[1:24]], axis=0)


def wave_terms():
    k = np.concatenate([np.arange(25), np.arange(1, 24)])
    return 4 * np.sin(np.pi * k / EXTENT) ** 2


def split_bf16(a):
    a = np.asarray(a, np.float32)
    hi = a.astype(jnp.bfloat16)
    lo = (a - hi.astype(np.float32)).astype(jnp.bfloat16)
    return hi, lo


Q = basis()
P2 = wave_terms()
WX = np.einsum("kx,zw->kzwx", Q, np.eye(8)).reshape(384, 384)
WX_HI, WX_LO = split_bf16(WX)
WXT_HI, WXT_LO = split_bf16(WX.T)
Q_HI, Q_LO = split_bf16(Q)
QT_HI, QT_LO = split_bf16(Q.T)
Q_STACK = np.concatenate([Q_HI, Q_HI, Q_LO], axis=1)
QT_STACK = np.concatenate([QT_HI, QT_HI, QT_LO], axis=1)
PZ = np.repeat(P2[:, None], 128, axis=1).astype(np.float32)
PX = P2.astype(np.float32)
PXM = np.repeat(np.repeat(P2.reshape(6, 1, 8), 6, axis=1).reshape(36, 8), 16, axis=1)
PZM = np.repeat(np.tile(P2.reshape(6, 8).T[:, None, :], (1, 6, 1)).reshape(8, 36, 1), 128, axis=2)
PSUM = (PXM[None] + PZM).astype(np.float32)


def zero_green(distance):
    d = np.arange(EXTENT)
    mean = np.mean(d * d / 96 - d / 2)
    return float(12 * (distance * distance / 96 - distance / 2 - mean))


def cmul(p, q):
    return (p[0] * q[0] - p[1] * q[1], p[0] * q[1] + p[1] * q[0])


def cmul_conj(p, q):
    return (p[0] * q[0] + p[1] * q[1], p[1] * q[0] - p[0] * q[1])


def cadd(p, q):
    return (p[0] + q[0], p[1] + q[1])


def csub(p, q):
    return (p[0] - q[0], p[1] - q[1])


def cross_conj(a, b):
    out = []
    for k in range(3):
        p = cmul(a[(k + 1) % 3], b[(k + 2) % 3])
        q = cmul(a[(k + 2) % 3], b[(k + 1) % 3])
        out.append((p[0] - q[0], q[1] - p[1]))
    return out


def algebra_of(u0, u1):
    u2 = cross_conj(u0, u1)
    return [
        u0[1][1] + u1[0][1],
        u0[1][0] - u1[0][0],
        u0[0][1] - u1[1][1],
        u0[2][1] + u2[0][1],
        u0[2][0] - u2[0][0],
        u1[2][1] + u2[1][1],
        u1[2][0] - u2[1][0],
        (u0[0][1] + u1[1][1] - 2.0 * u2[2][1]) * (1.0 / root_three),
    ]


def rotation_of(a):
    half = 0.5 * step_size
    a = [half * v for v in a]
    e = a[7] * (1.0 / root_three)
    diag = [a[2] + e, e - a[2], -2.0 * e]
    zero = jnp.zeros_like(a[0])
    x = [
        [(zero, diag[0]), (a[1], a[0]), (a[4], a[3])],
        [(-a[1], a[0]), (zero, diag[1]), (a[6], a[5])],
        [(-a[4], a[3]), (-a[6], a[5]), (zero, diag[2])],
    ]

    def entry(i, j):
        total = None
        for k in range(3):
            p, q = x[i][k], x[k][j]
            if i == k and k == j:
                term = (-p[1] * q[1], None)
            elif i == k:
                term = (-p[1] * q[1], p[1] * q[0])
            elif k == j:
                term = (-p[1] * q[1], p[0] * q[1])
            else:
                term = cmul(p, q)
            if total is None:
                total = term
            else:
                re = total[0] + term[0]
                if total[1] is None:
                    im = term[1]
                elif term[1] is None:
                    im = total[1]
                else:
                    im = total[1] + term[1]
                total = (re, im)
        re = 0.5 * total[0] + x[i][j][0] if i != j else 0.5 * total[0] + 1.0
        im = 0.5 * total[1] + x[i][j][1]
        return (re, im)

    m0 = [entry(0, j) for j in range(3)]
    m1 = [entry(1, j) for j in range(3)]
    inv = lax.rsqrt(sum(p[0] * p[0] + p[1] * p[1] for p in m0))
    r0 = [(p[0] * inv, p[1] * inv) for p in m0]
    corr = cmul_conj(m1[0], r0[0])
    for k in (1, 2):
        corr = cadd(corr, cmul_conj(m1[k], r0[k]))
    w = [csub(m1[k], cmul(corr, r0[k])) for k in range(3)]
    inv = lax.rsqrt(sum(p[0] * p[0] + p[1] * p[1] for p in w))
    r1 = [(p[0] * inv, p[1] * inv) for p in w]
    return r0, r1


def two_rows_of(load):
    u0 = [(load(2 * c), load(2 * c + 1)) for c in range(3)]
    u1 = [(load(6 + 2 * c), load(6 + 2 * c + 1)) for c in range(3)]
    return u0, u1


def project_kernel(links, hs):
    def project(q, carry):
        off = pl.multiple_of(q * 384, 128)
        for d in range(3):
            u0, u1 = two_rows_of(lambda n: links[12 * d + n, :, pl.ds(off, 384)])
            for c, h in enumerate(algebra_of(u0, u1)):
                hs[d * 8 + c, :, pl.ds(off, 384)] = h
        return carry

    lax.fori_loop(0, 9, project, 0)


def gradient_kernel(idx, hs, o0, o1, o2, o3, zb, ws):
    yc = idx[1]
    even = (yc % 2) == 0
    width = SITES + 128
    xzero = (lax.broadcasted_iota(jnp.int32, (8, SITES), 1) % EXTENT) == 0
    lane = lax.broadcasted_iota(jnp.int32, (8, 128), 1)
    first = lane < 48
    second = (lane >= 48) & (lane < 96)
    zeros = jnp.zeros((8, 128), f32)

    def combine(c, carry):
        hx = hs[c]
        hy = jnp.concatenate([hs[8 + c], zeros], axis=1)
        hz = hs[16 + c]
        zb[...] = pltpu.roll(jnp.concatenate([hz, zeros], axis=1), 48, 1)
        head = zb[:, 0:128]
        zb[:, 0:128] = jnp.where(second & even, pltpu.roll(hz[:, 2304:2432], 48, 1), head)
        zb[:, 2304:2432] = jnp.where(second & even, 0.0, zb[:, 2304:2432])
        zb[:, 1152:1280] = jnp.where(second & jnp.logical_not(even), 0.0, zb[:, 1152:1280])
        bx = jnp.where(xzero, pltpu.roll(hx, SITES - 47, 1), pltpu.roll(hx, 1, 1))
        near = (bx - hx) - hz - hs[8 + c]
        p = jnp.concatenate([near, zeros], axis=1) + zb[...]
        p = pltpu.roll(p, 80, 1)
        ha = pltpu.roll(hy, 80, 1)
        ws[c, :, 0:PLANE] = p[:, 0:PLANE]
        ws[c, :, PLANE:width] = p[:, PLANE:width] + ha[:, 0 : width - PLANE]
        ws[c, :, width:WINDOW] = ha[:, width - PLANE : width]
        wrap = jnp.where(even, hz[:, 0:128], hz[:, 1152:1280])
        ws[c, :, WIDE:WINDOW] += pltpu.roll(jnp.where(first, wrap, 0.0), 80, 1)
        return carry

    lax.fori_loop(0, 8, combine, 0)
    for k, o in enumerate((o0, o1, o2, o3)):
        o[...] = ws[pl.ds(2 * lax.rem(yc + k, 4), 2)]


def lambda_of(m):
    s = jnp.sqrt(m + 0.25 * m * m)
    return 1.0 / (1.0 + 0.5 * m + s), s


def split_value(a):
    hi = a.astype(bf16)
    return hi, (a - hi.astype(f32)).astype(bf16)


def dot(a, b, ca, cb):
    return lax.dot_general(a, b, (((ca,), (cb,)), ((), ())), preferred_element_type=f32)


def stack_of(a):
    hi, lo = split_value(a)
    return jnp.concatenate([hi, lo, hi], axis=0)


def decay_kernel(px, pz, after, lam_out, kap_out):
    def one(k, carry):
        lam, s = lambda_of(px[k] + pz[...])
        lam_out[k] = lam
        kap_out[k] = 6.0 / s
        return carry

    lax.fori_loop(0, EXTENT, one, 0)


def weight_kernel(px, pz, after, wa_out, wb_out):
    gi = lax.broadcasted_iota(jnp.int32, (EXTENT, 128), 1) // 16
    row = lax.broadcasted_iota(jnp.int32, (EXTENT, 128), 0)
    gr = 7 - gi

    def one(k, carry):
        lam, s = lambda_of(px[k] + pz[...])
        lam2 = lam * lam
        lam4 = lam2 * lam2
        wa = jnp.where(gi % 2 == 1, lam, 1.0) * jnp.where((gi // 2) % 2 == 1, lam2, 1.0)
        wa_out[k] = wa * jnp.where(gi >= 4, lam4, 1.0)
        wb = jnp.where(gr % 2 == 1, lam, 1.0) * jnp.where((gr // 2) % 2 == 1, lam2, 1.0)
        wb_out[k] = jnp.where((row == 0) & (k == 0), gi.astype(f32), wb * jnp.where(gr >= 4, lam4, 1.0))
        return carry

    lax.fori_loop(0, EXTENT, one, 0)


def forward_kernel(
    idx, r0, r1, r2, r3, wxh, wxl, qs, lamt, kapt, sout, own, e7o, e0o, e1o, e6o, theta, gs, ds, es
):
    yc = idx[1]
    lane = lax.broadcasted_iota(jnp.int32, (8, 128), 1)
    gs[...] = jnp.zeros((2, 8, GROUP), f32)
    for k, r in enumerate((r0, r1, r2, r3)):
        yd = lax.rem(yc - k + 4, 4)
        off = pl.multiple_of(yd * SITES + PLANE - 128, 128)
        off_end = pl.multiple_of(yd * SITES + PLANE - 128 + WIDE, 128)
        off_wrap = pl.multiple_of(yd * SITES + lax.rem(yd, 2) * 1152, 128)
        for f in range(2):
            gs[f, :, pl.ds(off, WIDE)] += r[f, :, 0:WIDE]
            tail = r[f, :, WIDE:WINDOW]
            gs[f, :, pl.ds(off_end, 128)] += jnp.where(lane < 80, tail, 0.0)
            gs[f, :, pl.ds(off_wrap, 128)] += jnp.where(lane < 48, pltpu.roll(tail, 48, 1), 0.0)

    def along_x(j, carry):
        pieces = []
        for half in range(2):
            for n in range(8):
                for f in range(2):
                    place = PLANE * n + 384 * (2 * j + half)
                    pieces.append(gs[f, :, pl.ds(pl.multiple_of(place, 128), 384)])
        bh, bl = split_value(jnp.concatenate(pieces, axis=0))
        wh = wxh[...]
        out = dot(wh, bh, 1, 1) + dot(wh, bl, 1, 1) + dot(wxl[...], bh, 1, 1)
        for half in range(2):
            place = pl.multiple_of(8 * (2 * j + half), 8)
            ds[:, pl.ds(place, 8), :] = out[:, 128 * half : 128 * half + 128].reshape(EXTENT, 8, 128)
        return carry

    lax.fori_loop(0, 3, along_x, 0)

    gi = lax.broadcasted_iota(jnp.int32, (EXTENT, 128), 1) // 16

    def along_z(m, squares):
        packs = [jnp.zeros((EXTENT, 128), f32) for _ in range(6)]
        pair = None
        for g in range(8):
            k = m * 8 + g
            if g % 2 == 0:
                pair = dot(qs[...], stack_of(jnp.concatenate([ds[k], ds[k + 1]], axis=1)), 1, 0)
            e = pair[:, 128 * (g % 2) : 128 * (g % 2) + 128]
            if g == 0:
                es[m] = e[0:8]
            lam = lamt[k]
            lam2 = lam * lam
            lam4 = lam2 * lam2
            up = e + jnp.where(gi >= 1, lam, 0.0) * pltpu.roll(e, 16, 1)
            up = up + jnp.where(gi >= 2, lam2, 0.0) * pltpu.roll(up, 32, 1)
            up = up + jnp.where(gi >= 4, lam4, 0.0) * pltpu.roll(up, 64, 1)
            down = e + jnp.where(gi <= 6, lam, 0.0) * pltpu.roll(e, 112, 1)
            down = down + jnp.where(gi <= 5, lam2, 0.0) * pltpu.roll(down, 96, 1)
            down = down + jnp.where(gi <= 3, lam4, 0.0) * pltpu.roll(down, 64, 1)
            own[k] = kapt[k] * (up + down - e)
            squares = squares + sum(e[8 * i : 8 * i + 8] * e[8 * i : 8 * i + 8] for i in range(6))
            for n, (v, source) in enumerate(((up, 7), (down, 0), (e, 7), (e, 0), (e, 1), (e, 6))):
                shift = ((g - source) * 16) % 128
                packs[n] = jnp.where(gi == g, pltpu.roll(v, shift, 1) if shift else v, packs[n])
        for i in range(6):
            sout[pl.ds(m * 6 + i, 8, stride=72), :] = packs[0][8 * i : 8 * i + 8]
            sout[pl.ds(36 + m * 6 + i, 8, stride=72), :] = packs[1][8 * i : 8 * i + 8]
        e7o[m] = packs[2]
        e0o[m] = packs[3]
        e1o[m] = packs[4]
        e6o[m] = packs[5]
        return squares

    squares = lax.fori_loop(0, 6, along_z, jnp.zeros((8, 128), f32))

    e0 = es[0]
    gt = lane // 16
    row = lax.broadcasted_iota(jnp.int32, (8, 128), 0)
    total = zero_green(0) * e0
    for n in range(1, 8):
        weight = jnp.where(gt >= n, zero_green(n), zero_green(8 - n))
        total = total + weight * pltpu.roll(e0, 16 * n, 1)
    own[0, 0:8, :] = jnp.where(row == 0, total, own[0, 0:8, :])
    theta[...] = jnp.where((gt >= 2) & (gt <= 5), squares, 0.0)
    yf = gt.astype(f32)

    def over_groups(v):
        for n in (16, 32, 64):
            v = v + pltpu.roll(v, n, 1)
        return v

    m1 = over_groups(yf * e0)
    m2 = over_groups(yf * yf * e0)
    here = (row == 0) & (gt == 0)
    sout[0:8, :] = jnp.where(here, m1, sout[0:8, :])
    sout[36:44, :] = jnp.where(here, m2, sout[36:44, :])


def solve_kernel(idx, s, psum, before, after, e1, e6, theta_in, out, theta):
    zc = idx[0]
    squares = theta_in[...]
    for m in range(6):
        for i in range(6):
            plane_first = e1[m, 8 * i : 8 * i + 8] + before[m, 8 * i : 8 * i + 8]
            plane_last = e6[m, 8 * i : 8 * i + 8] + after[m, 8 * i : 8 * i + 8]
            squares = squares + plane_first * plane_first + plane_last * plane_last
    theta[...] = squares
    lam, root = lambda_of(psum[zc])
    lam2 = lam * lam
    lam6 = lam2 * lam2 * lam2
    lam12 = lam6 * lam6
    lam24 = lam12 * lam12
    row = lax.broadcasted_iota(jnp.int32, (36, 128), 0)
    lane = lax.broadcasted_iota(jnp.int32, (36, 128), 1)
    zero = (row == 0) & (lane < 16) & (zc == 0)
    kappa = 6.0 / root / (1.0 - lam24 * lam24)
    coef = []
    power = 1.0 + 0.5 * psum[zc] + root
    for k in range(1, 9):
        coef.append(kappa * power)
        power = power * lam6
    plus = [s[72 * n : 72 * n + 36, :] for n in range(8)]
    minus = [s[72 * n + 36 : 72 * n + 72, :] for n in range(8)]
    total_p = sum(plus)
    total_m = sum(minus)
    coef_a = [jnp.where(zero, 12.0 * (0.5 - k / 8.0) if k < 8 else 0.0, coef[k - 1]) for k in range(1, 9)]
    for t in range(8):
        a = coef_a[0] * plus[(t - 1) % 8]
        b = coef[0] * minus[(t + 1) % 8]
        for k in range(2, 9):
            a = a + coef_a[k - 1] * plus[(t - k) % 8]
            b = b + coef[k - 1] * minus[(t + k) % 8]
        a = a + jnp.where(zero, 0.125 * (total_m - minus[t]), 0.0)
        b = jnp.where(zero, -0.25 * (total_p - plus[t]), b)
        out[72 * t : 72 * t + 36, :] = a
        out[72 * t + 36 : 72 * t + 72, :] = b


def spread_groups(v, gi):
    level = [v]
    for width in (4, 2, 1):
        bit = (gi // width) % 2
        out = []
        for a in level:
            if width == 4:
                rolled = pltpu.roll(a, 64, 1)
            else:
                up = pltpu.roll(a, 16 * width, 1)
                down = pltpu.roll(a, 128 - 16 * width, 1)
                rolled = jnp.where(bit == 0, down, up)
            out.append(jnp.where(bit == 0, a, rolled))
            out.append(jnp.where(bit == 0, rolled, a))
        level = out
    return level


def backward_kernel(
    idx, ab, own, wxth, wxtl, qts, wat, wbt, before, after, o0, o1, o2, o3, ds, gs
):
    yc = idx[1]
    gi = lax.broadcasted_iota(jnp.int32, (EXTENT, 128), 1) // 16

    def along_z(m, carry):
        ta = jnp.concatenate([ab[pl.ds(m * 6 + i, 8, stride=72), :] for i in range(6)], axis=0)
        tb = jnp.concatenate([ab[pl.ds(36 + m * 6 + i, 8, stride=72), :] for i in range(6)], axis=0)
        las = spread_groups(ta, gi)
        lbs = spread_groups(tb, gi)
        prior = -12.0 * before[m]
        later = -12.0 * after[m]
        u = []
        for g in range(8):
            k = m * 8 + g
            v = own[k] + las[g] * wat[k] + lbs[g] * wbt[k]
            shift = ((7 - g) * 16) % 128
            edge = jnp.where(gi == 0, pltpu.roll(prior, (-g * 16) % 128, 1) if g else prior, 0.0)
            edge = jnp.where(gi == 7, pltpu.roll(later, shift, 1) if shift else later, edge)
            u.append(v + edge)
            if g % 2 == 1:
                pair = dot(qts[...], stack_of(jnp.concatenate(u, axis=1)), 1, 0)
                ds[k - 1] = pair[:, 0:128]
                ds[k] = pair[:, 128:256]
                u = []
        return carry

    lax.fori_loop(0, 6, along_z, 0)

    def along_x(j, carry):
        halves = []
        for half in range(2):
            place = pl.multiple_of(8 * (2 * j + half), 8)
            halves.append(ds[:, pl.ds(place, 8), :].reshape(384, 128))
        dh, dl = split_value(jnp.concatenate(halves, axis=1))
        wh = wxth[...]
        o = dot(wh, dh, 1, 0) + dot(wh, dl, 1, 0) + dot(wxtl[...], dh, 1, 0)
        for half in range(2):
            t = jnp.transpose(o[:, 128 * half : 128 * half + 128])
            for n in range(8):
                for f in range(2):
                    place = PLANE * n + 384 * (2 * j + half)
                    gs[f, :, pl.ds(pl.multiple_of(place, 128), 384)] = t[16 * n + 8 * f : 16 * n + 8 * f + 8]
        return carry

    lax.fori_loop(0, 3, along_x, 0)
    for k, out in enumerate((o0, o1, o2, o3)):
        yd = lax.rem(yc + k, 4)
        off = pl.multiple_of(yd * SITES + PLANE - 128, 128)
        off_extra = pl.multiple_of(yd * SITES + lax.rem(yd, 2) * 1152, 128)
        for f in range(2):
            out[f, :, 0:WIDE] = pltpu.roll(gs[f, :, pl.ds(off, WINDOW)], WIDE + 48, 1)[:, 0:WIDE]
            out[f, :, WIDE:WINDOW] = gs[f, :, pl.ds(off_extra, 128)]


def rotate_kernel(idx, r0, r1, r2, r3, theta, links, out, stats, sm, ex, gs, fix, deficit):
    yc = idx[1]
    even = (yc % 2) == 0
    lane = lax.broadcasted_iota(jnp.int32, (8, 128), 1)
    for k, r in enumerate((r0, r1, r2, r3)):
        c0 = 2 * lax.rem(yc - k + 4, 4)
        for f in range(2):
            sm[c0 + f] = r[f, :, 0:WIDE]
            ex[c0 + f] = r[f, :, WIDE : WIDE + 128]

    def store_rotation(load, store):
        g0, g1 = rotation_of([load(c) for c in range(8)])
        g2 = cross_conj(g0, g1)
        for i, g in enumerate((g0, g1, g2)):
            for c in range(3):
                for p in range(2):
                    store(6 * i + 2 * c + p, g[c][p])

    def rotations(q, carry):
        off = pl.multiple_of(q * 384, 128)

        def store(n, v):
            gs[n, :, pl.ds(off, 384)] = v

        store_rotation(lambda c: sm[c, :, pl.ds(off, 384)], store)
        return carry

    lax.fori_loop(0, 15, rotations, 0)

    def store_fix(n, v):
        fix[0, n] = v

    store_rotation(lambda c: ex[c], store_fix)
    for n in range(18):
        fix[1, n] = pltpu.roll(gs[n, :, 0:128], 80, 1)
    deficit[...] = jnp.zeros((8, 128), f32)
    xlast = (lax.broadcasted_iota(jnp.int32, (8, 384), 1) % EXTENT) == EXTENT - 1

    def products(q, carry):
        off = pl.multiple_of(q * 384, 128)
        far = pl.multiple_of(q * 384 + PLANE, 128)
        from_fix = ((q == 0) & even) | ((q == 3) & jnp.logical_not(even)) | ((q == 6) & even)
        which = jnp.where(q == 6, 1, 0)
        head = (lane < 48) & from_fix

        def here(n):
            return gs[n, :, pl.ds(off, 384)]

        def ahead_x(n):
            v = here(n)
            return jnp.where(xlast, pltpu.roll(v, 47, 1), pltpu.roll(v, 383, 1))

        def ahead_y(n):
            return gs[n, :, pl.ds(far, 384)]

        def ahead_z(n):
            v = pltpu.roll(gs[n, :, pl.ds(off, 512)], 512 - 48, 1)[:, 0:384]
            return jnp.concatenate([jnp.where(head, fix[which, n], v[:, 0:128]), v[:, 128:384]], axis=1)

        def matrix(load):
            return [[(load(6 * i + 2 * c), load(6 * i + 2 * c + 1)) for c in range(3)] for i in range(3)]

        g = matrix(here)
        acc = jnp.zeros((8, 384), f32)
        for d, ahead in enumerate((ahead_x, ahead_y, ahead_z)):
            u0, u1 = two_rows_of(lambda n: links[12 * d + n, :, pl.ds(off, 384)])
            u = [u0, u1, cross_conj(u0, u1)]
            h = matrix(ahead)
            rows_out = []
            for i in range(2):
                t = []
                for j in range(3):
                    v = cmul(g[i][0], u[0][j])
                    for k in (1, 2):
                        v = cadd(v, cmul(g[i][k], u[k][j]))
                    t.append(v)
                line = []
                for j in range(3):
                    v = cmul_conj(t[0], h[j][0])
                    for k in (1, 2):
                        v = cadd(v, cmul_conj(t[k], h[j][k]))
                    line.append(v)
                    out[12 * d + 6 * i + 2 * j, :, pl.ds(off, 384)] = v[0]
                    out[12 * d + 6 * i + 2 * j + 1, :, pl.ds(off, 384)] = v[1]
                rows_out.append(line)
            a, b = rows_out
            corner = (a[0][0] * b[1][0] - a[0][1] * b[1][1]) - (a[1][0] * b[0][0] - a[1][1] * b[0][1])
            acc = acc + (3.0 - a[0][0] - b[1][0] - corner)
        deficit[...] += acc[:, 0:128] + acc[:, 128:256] + acc[:, 256:384]
        return carry

    lax.fori_loop(0, 9, products, 0)
    row = lax.broadcasted_iota(jnp.int32, (8, 128), 0)
    line = jnp.sum(jnp.where(row == lane, jnp.sum(deficit[...], axis=1, keepdims=True), 0.0), axis=0, keepdims=True)
    total = jnp.sum(jnp.sum(theta[...], axis=1, keepdims=True), axis=0, keepdims=True)
    line = jnp.where(lane[0:1] == 8, total, line)
    stats[...] = jnp.broadcast_to(line, (32, 128))


def shape(*dims):
    return jax.ShapeDtypeStruct(dims, f32)


def call(kernel, outs, scalars, scratch=()):
    def run(*args):
        vm = pl.BlockSpec(memory_space=pltpu.VMEM)
        sm = pl.BlockSpec(memory_space=pltpu.SMEM)
        return pl.pallas_call(
            kernel,
            in_specs=[sm] * scalars + [vm] * (len(args) - scalars),
            out_specs=[vm] * len(outs),
            out_shape=list(outs),
            scratch_shapes=list(scratch),
            compiler_params=pltpu.CompilerParams(vmem_limit_bytes=24 * 1024 * 1024),
        )(*args)

    return run


def exchange_y(pieces):
    return [pieces[0]] + [from_behind(pieces[k], "space_1", k) for k in (1, 2, 3)]


def exchange_z(a):
    return lax.all_to_all(a, "space_0", split_axis=0, concat_axis=0, tiled=True)


def body(links):
    zc = lax.axis_index("space_0")
    yc = lax.axis_index("space_1")
    idx = jnp.stack([zc, yc]).astype(jnp.int32)
    px = jnp.asarray(PX)
    flat = links.transpose(1, 2, 3, 4, 0, 5).reshape(36, SLICES, SITES)
    window = shape(2, 8, WINDOW)
    modes = shape(48, 48, 128)
    packed = shape(6, 48, 128)
    (hs,) = call(project_kernel, [shape(24, 8, SITES)], 0)(flat)
    pieces = call(
        gradient_kernel,
        [window] * 4,
        1,
        [pltpu.VMEM((8, SITES + 128), f32), pltpu.VMEM((8, 8, WINDOW), f32)],
    )(idx, hs)
    r = exchange_y(pieces)
    lam, kap = call(decay_kernel, [modes] * 2, 1)(px, jnp.asarray(PZ), hs)
    moments, own, e7, e0, e1, e6, theta = call(
        forward_kernel,
        [shape(576, 128), modes, packed, packed, packed, packed, shape(8, 128)],
        1,
        [pltpu.VMEM((2, 8, GROUP), f32), pltpu.VMEM((48, 48, 128), f32), pltpu.VMEM((6, 8, 128), f32)],
    )(idx, *r, jnp.asarray(WX_HI), jnp.asarray(WX_LO), jnp.asarray(Q_STACK), lam, kap)
    before = from_behind(e7, "space_0", 1)
    after = from_behind(e0, "space_0", -1)
    moments = exchange_z(moments)
    amps, theta = call(solve_kernel, [shape(576, 128), shape(8, 128)], 1)(
        idx, moments, jnp.asarray(PSUM), before, after, e1, e6, theta
    )
    wa, wb = call(weight_kernel, [modes] * 2, 1)(px, jnp.asarray(PZ), amps)
    theta = theta + from_behind(theta, "tm_1", 1)
    theta = theta + sum(from_behind(theta, "tm_0", k) for k in (1, 2, 3))
    amps = exchange_z(amps)
    windows = call(
        backward_kernel,
        [window] * 4,
        1,
        [pltpu.VMEM((48, 48, 128), f32), pltpu.VMEM((2, 8, GROUP), f32)],
    )(
        idx, amps, own, jnp.asarray(WXT_HI), jnp.asarray(WXT_LO), jnp.asarray(QT_STACK), wa, wb,
        before, after,
    )
    r = exchange_y(windows)
    new_flat, stats = call(
        rotate_kernel,
        [shape(36, 8, SITES), shape(32, 128)],
        1,
        [
            pltpu.VMEM((8, 8, WIDE), f32),
            pltpu.VMEM((8, 8, 128), f32),
            pltpu.VMEM((18, 8, WIDE), f32),
            pltpu.VMEM((2, 18, 8, 128), f32),
            pltpu.VMEM((8, 128), f32),
        ],
    )(idx, *r, theta, flat)
    new_links = new_flat.reshape(3, 2, 3, 2, SLICES, SITES).transpose(4, 0, 1, 2, 3, 5)
    both = jnp.sum(lax.all_to_all(stats, SPACE, split_axis=0, concat_axis=0, tiled=True), axis=0)
    theta = both[8] / (SLICES * 8 * EXTENT**3)
    deficit = both[:8] / EXTENT**3
    return (new_links, theta, deficit)


def solution(mesh):
    torus = Mesh(mesh.devices.reshape(4, 2, 8, 4), ("tm_0", "tm_1", "space_0", "space_1"))
    in_specs = (P(TM, None, None, None, None, SPACE),)
    out_specs = (P(TM, None, None, None, None, SPACE), P(), P(TM))
    return jax.shard_map(body, mesh=torus, in_specs=in_specs, out_specs=out_specs, check_vma=False)
```

```python
import functools
import math

import jax
import jax.numpy as jnp
import numpy as np
from jax import lax
from jax.experimental import pallas as pl
from jax.experimental.pallas import tpu as pltpu
from jax.sharding import Mesh
from jax.sharding import PartitionSpec as P

EXTENT = 48
SPACE = ("space_0", "space_1")
TM = ("tm_0", "tm_1")
TM_SPACE = ("tm_0", "tm_1", "space_0", "space_1")
SLICES = 8
ROWS = 72
SITES = ROWS * EXTENT
PLANE = EXTENT * EXTENT
WIDE = SITES + PLANE
WINDOW = WIDE + 128
BLOCK = 72
GROUP = 8 * PLANE

root_three = math.sqrt(3.0)
step_size = 0.08
f32 = jnp.float32
bf16 = jnp.bfloat16


def from_behind(block, axis, distance):
    n = lax.axis_size(axis)
    return lax.ppermute(block, axis, [((i - distance) % n, i) for i in range(n)])


def basis():
    k = np.arange(25)[:, None]
    x = np.arange(EXTENT)[None, :]
    cos = np.cos(2 * np.pi * k * x / EXTENT) * math.sqrt(2 / EXTENT)
    cos[0] /= math.sqrt(2)
    cos[24] /= math.sqrt(2)
    sin = np.sin(2 * np.pi * k * x / EXTENT) * math.sqrt(2 / EXTENT)
    return np.concatenate([cos, sin[1:24]], axis=0)


def wave_terms():
    k = np.concatenate([np.arange(25), np.arange(1, 24)])
    return 4 * np.sin(np.pi * k / EXTENT) ** 2


def split_bf16(a):
    a = np.asarray(a, np.float32)
    hi = a.astype(jnp.bfloat16)
    lo = (a - hi.astype(np.float32)).astype(jnp.bfloat16)
    return hi, lo


Q = basis()
P2 = wave_terms()
Q_HI, Q_LO = split_bf16(Q)
QT_HI, QT_LO = split_bf16(Q.T)
Q_STACK = np.concatenate([Q_HI, Q_HI, Q_LO], axis=1)
QT_STACK = np.concatenate([QT_HI, QT_HI, QT_LO], axis=1)
PZ = np.repeat(P2[:, None], 128, axis=1).astype(np.float32)
PX = P2.astype(np.float32)
PXM = np.repeat(np.repeat(P2.reshape(6, 1, 8), 6, axis=1).reshape(36, 8), 16, axis=1)
PZM = np.repeat(np.tile(P2.reshape(6, 8).T[:, None, :], (1, 6, 1)).reshape(8, 36, 1), 128, axis=2)
PSUM = (PXM[None] + PZM).astype(np.float32)


def zero_green(distance):
    d = np.arange(EXTENT)
    mean = np.mean(d * d / 96 - d / 2)
    return float(12 * (distance * distance / 96 - distance / 2 - mean))


def cmul(p, q):
    return (p[0] * q[0] - p[1] * q[1], p[0] * q[1] + p[1] * q[0])


def cmul_conj(p, q):
    return (p[0] * q[0] + p[1] * q[1], p[1] * q[0] - p[0] * q[1])


def cadd(p, q):
    return (p[0] + q[0], p[1] + q[1])


def csub(p, q):
    return (p[0] - q[0], p[1] - q[1])


def cross_conj(a, b):
    out = []
    for k in range(3):
        p = cmul(a[(k + 1) % 3], b[(k + 2) % 3])
        q = cmul(a[(k + 2) % 3], b[(k + 1) % 3])
        out.append((p[0] - q[0], q[1] - p[1]))
    return out


def algebra_of(u0, u1):
    u2 = cross_conj(u0, u1)
    return [
        u0[1][1] + u1[0][1],
        u0[1][0] - u1[0][0],
        u0[0][1] - u1[1][1],
        u0[2][1] + u2[0][1],
        u0[2][0] - u2[0][0],
        u1[2][1] + u2[1][1],
        u1[2][0] - u2[1][0],
        (u0[0][1] + u1[1][1] - 2.0 * u2[2][1]) * (1.0 / root_three),
    ]


def rotation_of(a):
    half = 0.5 * step_size
    a = [half * v for v in a]
    e = a[7] * (1.0 / root_three)
    diag = [a[2] + e, e - a[2], -2.0 * e]
    zero = jnp.zeros_like(a[0])
    x = [
        [(zero, diag[0]), (a[1], a[0]), (a[4], a[3])],
        [(-a[1], a[0]), (zero, diag[1]), (a[6], a[5])],
        [(-a[4], a[3]), (-a[6], a[5]), (zero, diag[2])],
    ]

    def entry(i, j):
        total = None
        for k in range(3):
            p, q = x[i][k], x[k][j]
            if i == k and k == j:
                term = (-p[1] * q[1], None)
            elif i == k:
                term = (-p[1] * q[1], p[1] * q[0])
            elif k == j:
                term = (-p[1] * q[1], p[0] * q[1])
            else:
                term = cmul(p, q)
            if total is None:
                total = term
            else:
                re = total[0] + term[0]
                if total[1] is None:
                    im = term[1]
                elif term[1] is None:
                    im = total[1]
                else:
                    im = total[1] + term[1]
                total = (re, im)
        re = 0.5 * total[0] + x[i][j][0] if i != j else 0.5 * total[0] + 1.0
        im = 0.5 * total[1] + x[i][j][1]
        return (re, im)

    m0 = [entry(0, j) for j in range(3)]
    m1 = [entry(1, j) for j in range(3)]
    inv = lax.rsqrt(sum(p[0] * p[0] + p[1] * p[1] for p in m0))
    r0 = [(p[0] * inv, p[1] * inv) for p in m0]
    corr = cmul_conj(m1[0], r0[0])
    for k in (1, 2):
        corr = cadd(corr, cmul_conj(m1[k], r0[k]))
    w = [csub(m1[k], cmul(corr, r0[k])) for k in range(3)]
    inv = lax.rsqrt(sum(p[0] * p[0] + p[1] * p[1] for p in w))
    r1 = [(p[0] * inv, p[1] * inv) for p in w]
    return r0, r1


def two_rows_of(load):
    u0 = [(load(2 * c), load(2 * c + 1)) for c in range(3)]
    u1 = [(load(6 + 2 * c), load(6 + 2 * c + 1)) for c in range(3)]
    return u0, u1


def project_kernel(links, hs):
    def project(q, carry):
        off = pl.multiple_of(q * 384, 128)
        for d in range(3):
            u0, u1 = two_rows_of(lambda n: links[12 * d + n, :, pl.ds(off, 384)])
            for c, h in enumerate(algebra_of(u0, u1)):
                hs[d * 8 + c, :, pl.ds(off, 384)] = h
        return carry

    lax.fori_loop(0, 9, project, 0)


def gradient_kernel(shift, idx, hs, out, zb):
    yc = idx[1]
    even = (yc % 2) == 0
    width = SITES + 128
    xzero = (lax.broadcasted_iota(jnp.int32, (8, SITES), 1) % EXTENT) == 0
    lane = lax.broadcasted_iota(jnp.int32, (8, 128), 1)
    first = lane < 48
    second = (lane >= 48) & (lane < 96)
    zeros = jnp.zeros((8, 128), f32)

    def combine(f, carry):
        c = 2 * lax.rem(yc + shift, 4) + f
        hx = hs[c]
        hy = jnp.concatenate([hs[8 + c], zeros], axis=1)
        hz = hs[16 + c]
        zb[...] = pltpu.roll(jnp.concatenate([hz, zeros], axis=1), 48, 1)
        head = zb[:, 0:128]
        zb[:, 0:128] = jnp.where(second & even, pltpu.roll(hz[:, 2304:2432], 48, 1), head)
        zb[:, 2304:2432] = jnp.where(second & even, 0.0, zb[:, 2304:2432])
        zb[:, 1152:1280] = jnp.where(second & jnp.logical_not(even), 0.0, zb[:, 1152:1280])
        bx = jnp.where(xzero, pltpu.roll(hx, SITES - 47, 1), pltpu.roll(hx, 1, 1))
        near = (bx - hx) - hz - hs[8 + c]
        p = jnp.concatenate([near, zeros], axis=1) + zb[...]
        p = pltpu.roll(p, 80, 1)
        ha = pltpu.roll(hy, 80, 1)
        out[f, :, 0:PLANE] = p[:, 0:PLANE]
        out[f, :, PLANE:width] = p[:, PLANE:width] + ha[:, 0 : width - PLANE]
        out[f, :, width:WINDOW] = ha[:, width - PLANE : width]
        wrap = jnp.where(even, hz[:, 0:128], hz[:, 1152:1280])
        out[f, :, WIDE:WINDOW] += pltpu.roll(jnp.where(first, wrap, 0.0), 80, 1)
        return carry

    for f in range(2):
        combine(f, 0)


def lambda_of(m):
    s = jnp.sqrt(m + 0.25 * m * m)
    return 1.0 / (1.0 + 0.5 * m + s), s


def split_value(a):
    hi = a.astype(bf16)
    return hi, (a - hi.astype(f32)).astype(bf16)


def dot(a, b, ca, cb):
    return lax.dot_general(a, b, (((ca,), (cb,)), ((), ())), preferred_element_type=f32)


def stack_of(a):
    hi, lo = split_value(a)
    return jnp.concatenate([hi, lo, hi], axis=0)


def decay_kernel(px, pz, after, lam_out, kap_out):
    def one(k, carry):
        lam, s = lambda_of(px[k] + pz[...])
        lam_out[k] = lam
        kap_out[k] = 6.0 / s
        return carry

    lax.fori_loop(0, EXTENT, one, 0)


def weight_kernel(px, pz, after, wa_out, wb_out):
    gi = lax.broadcasted_iota(jnp.int32, (EXTENT, 128), 1) // 16
    row = lax.broadcasted_iota(jnp.int32, (EXTENT, 128), 0)
    gr = 7 - gi

    def one(k, carry):
        lam, s = lambda_of(px[k] + pz[...])
        lam2 = lam * lam
        lam4 = lam2 * lam2
        wa = jnp.where(gi % 2 == 1, lam, 1.0) * jnp.where((gi // 2) % 2 == 1, lam2, 1.0)
        wa_out[k] = wa * jnp.where(gi >= 4, lam4, 1.0)
        wb = jnp.where(gr % 2 == 1, lam, 1.0) * jnp.where((gr // 2) % 2 == 1, lam2, 1.0)
        wb_out[k] = jnp.where((row == 0) & (k == 0), gi.astype(f32), wb * jnp.where(gr >= 4, lam4, 1.0))
        return carry

    lax.fori_loop(0, EXTENT, one, 0)


def matrix_kernel(qh, ql, qth, qtl, after, wxh, wxl, wxth, wxtl):
    def where_one(cond):
        return jnp.where(cond, 1.0, 0.0).astype(bf16)

    tall = lax.broadcasted_iota(jnp.int32, (384, EXTENT), 0)
    narrow = lax.broadcasted_iota(jnp.int32, (384, EXTENT), 1)
    wide = lax.broadcasted_iota(jnp.int32, (EXTENT, 384), 1)
    short = lax.broadcasted_iota(jnp.int32, (EXTENT, 384), 0)
    row = lax.broadcasted_iota(jnp.int32, (384, 384), 0)
    col = lax.broadcasted_iota(jnp.int32, (384, 384), 1)
    mask = (row % 8) == (col // EXTENT)
    mask_t = (row // EXTENT) == (col % 8)
    from_k = where_one(tall // 8 == narrow)
    to_x = where_one(wide % EXTENT == short)
    from_x = where_one(tall % EXTENT == narrow)
    to_k = where_one(wide // 8 == short)
    for q, out in ((qh, wxh), (ql, wxl)):
        a = dot(from_k, q[...], 1, 0).astype(bf16)
        out[...] = jnp.where(mask, dot(a, to_x, 1, 0), 0.0).astype(bf16)
    for q, out in ((qth, wxth), (qtl, wxtl)):
        a = dot(from_x, q[...], 1, 0).astype(bf16)
        out[...] = jnp.where(mask_t, dot(a, to_k, 1, 0), 0.0).astype(bf16)


def forward_kernel(
    idx, r0, r1, r2, r3, wxh, wxl, qs, lamt, kapt, m0, m1, m2, m3, m4, m5, m6, m7, own, e1o, e6o, theta, gs, ds, es, sout
):
    zc = idx[0]
    yc = idx[1]
    lane = lax.broadcasted_iota(jnp.int32, (8, 128), 1)
    gs[...] = jnp.zeros((2, 8, GROUP), f32)
    for k, r in enumerate((r0, r1, r2, r3)):
        yd = lax.rem(yc - k + 4, 4)
        off = pl.multiple_of(yd * SITES + PLANE - 128, 128)
        off_end = pl.multiple_of(yd * SITES + PLANE - 128 + WIDE, 128)
        off_wrap = pl.multiple_of(yd * SITES + lax.rem(yd, 2) * 1152, 128)
        for f in range(2):
            gs[f, :, pl.ds(off, WIDE)] += r[f, :, 0:WIDE]
            tail = r[f, :, WIDE:WINDOW]
            gs[f, :, pl.ds(off_end, 128)] += jnp.where(lane < 80, tail, 0.0)
            gs[f, :, pl.ds(off_wrap, 128)] += jnp.where(lane < 48, pltpu.roll(tail, 48, 1), 0.0)

    def along_x(j, carry):
        pieces = []
        for half in range(2):
            for n in range(8):
                for f in range(2):
                    place = PLANE * n + 384 * (2 * j + half)
                    pieces.append(gs[f, :, pl.ds(pl.multiple_of(place, 128), 384)])
        bh, bl = split_value(jnp.concatenate(pieces, axis=0))
        wh = wxh[...]
        out = dot(wh, bh, 1, 1) + dot(wh, bl, 1, 1) + dot(wxl[...], bh, 1, 1)
        for half in range(2):
            place = pl.multiple_of(8 * (2 * j + half), 8)
            ds[:, pl.ds(place, 8), :] = out[:, 128 * half : 128 * half + 128].reshape(EXTENT, 8, 128)
        return carry

    lax.fori_loop(0, 3, along_x, 0)

    gi = lax.broadcasted_iota(jnp.int32, (EXTENT, 128), 1) // 16

    def along_z(m, squares):
        packs = [jnp.zeros((EXTENT, 128), f32) for _ in range(6)]
        pair = None
        for g in range(8):
            k = m * 8 + g
            if g % 2 == 0:
                pair = dot(qs[...], stack_of(jnp.concatenate([ds[k], ds[k + 1]], axis=1)), 1, 0)
            e = pair[:, 128 * (g % 2) : 128 * (g % 2) + 128]
            if g == 0:
                es[m] = e[0:8]
            lam = lamt[k]
            lam2 = lam * lam
            lam4 = lam2 * lam2
            up = e + jnp.where(gi >= 1, lam, 0.0) * pltpu.roll(e, 16, 1)
            up = up + jnp.where(gi >= 2, lam2, 0.0) * pltpu.roll(up, 32, 1)
            up = up + jnp.where(gi >= 4, lam4, 0.0) * pltpu.roll(up, 64, 1)
            down = e + jnp.where(gi <= 6, lam, 0.0) * pltpu.roll(e, 112, 1)
            down = down + jnp.where(gi <= 5, lam2, 0.0) * pltpu.roll(down, 96, 1)
            down = down + jnp.where(gi <= 3, lam4, 0.0) * pltpu.roll(down, 64, 1)
            own[k] = kapt[k] * (up + down - e)
            squares = squares + sum(e[8 * i : 8 * i + 8] * e[8 * i : 8 * i + 8] for i in range(6))
            for n, (v, source) in enumerate(((up, 7), (down, 0), (e, 7), (e, 0), (e, 1), (e, 6))):
                shift = ((g - source) * 16) % 128
                packs[n] = jnp.where(gi == g, pltpu.roll(v, shift, 1) if shift else v, packs[n])
        for i in range(6):
            sout[pl.ds(m * 6 + i, 8, stride=72), :] = packs[0][8 * i : 8 * i + 8]
            sout[pl.ds(36 + m * 6 + i, 8, stride=72), :] = packs[1][8 * i : 8 * i + 8]
        m1[pl.ds(pl.multiple_of(BLOCK + 48 * m, 8), 48)] = packs[2]
        m7[pl.ds(pl.multiple_of(BLOCK + 48 * m, 8), 48)] = packs[3]
        e1o[m] = packs[4]
        e6o[m] = packs[5]
        return squares

    squares = lax.fori_loop(0, 6, along_z, jnp.zeros((8, 128), f32))

    e0 = es[0]
    gt = lane // 16
    row = lax.broadcasted_iota(jnp.int32, (8, 128), 0)
    total = zero_green(0) * e0
    for n in range(1, 8):
        weight = jnp.where(gt >= n, zero_green(n), zero_green(8 - n))
        total = total + weight * pltpu.roll(e0, 16 * n, 1)
    own[0, 0:8, :] = jnp.where(row == 0, total, own[0, 0:8, :])
    theta[...] = jnp.where((gt >= 2) & (gt <= 5), squares, 0.0)
    yf = gt.astype(f32)

    def over_groups(v):
        for n in (16, 32, 64):
            v = v + pltpu.roll(v, n, 1)
        return v

    first = over_groups(yf * e0)
    second = over_groups(yf * yf * e0)
    here = (row == 0) & (gt == 0)
    sout[0:8, :] = jnp.where(here, first, sout[0:8, :])
    sout[36:44, :] = jnp.where(here, second, sout[36:44, :])
    for k, o in enumerate((m0, m1, m2, m3, m4, m5, m6, m7)):
        o[0:BLOCK] = sout[pl.ds(pl.multiple_of(BLOCK * lax.rem(zc + k, 8), 8), BLOCK)]


def gather_z(zc, blocks, s):
    for k, r in enumerate(blocks):
        s[pl.ds(pl.multiple_of(BLOCK * lax.rem(zc - k + 8, 8), 8), BLOCK)] = r[0:BLOCK]


def solve_kernel(
    idx, r0, r1, r2, r3, r4, r5, r6, r7, psum, e1, e6, theta_in, o0, o1, o2, o3, o4, o5, o6, o7, theta, s, out
):
    zc = idx[0]
    gather_z(zc, (r0, r1, r2, r3, r4, r5, r6, r7), s)
    squares = theta_in[...]
    for m in range(6):
        for i in range(6):
            place = BLOCK + 48 * m + 8 * i
            plane_first = e1[m, 8 * i : 8 * i + 8] + r1[place : place + 8]
            plane_last = e6[m, 8 * i : 8 * i + 8] + r7[place : place + 8]
            squares = squares + plane_first * plane_first + plane_last * plane_last
    theta[...] = squares
    lam, root = lambda_of(psum[zc])
    lam2 = lam * lam
    lam6 = lam2 * lam2 * lam2
    lam12 = lam6 * lam6
    lam24 = lam12 * lam12
    row = lax.broadcasted_iota(jnp.int32, (36, 128), 0)
    lane = lax.broadcasted_iota(jnp.int32, (36, 128), 1)
    zero = (row == 0) & (lane < 16) & (zc == 0)
    kappa = 6.0 / root / (1.0 - lam24 * lam24)
    coef = []
    power = 1.0 + 0.5 * psum[zc] + root
    for k in range(1, 9):
        coef.append(kappa * power)
        power = power * lam6
    plus = [s[72 * n : 72 * n + 36, :] for n in range(8)]
    minus = [s[72 * n + 36 : 72 * n + 72, :] for n in range(8)]
    total_p = sum(plus)
    total_m = sum(minus)
    coef_a = [jnp.where(zero, 12.0 * (0.5 - k / 8.0) if k < 8 else 0.0, coef[k - 1]) for k in range(1, 9)]
    for t in range(8):
        a = coef_a[0] * plus[(t - 1) % 8]
        b = coef[0] * minus[(t + 1) % 8]
        for k in range(2, 9):
            a = a + coef_a[k - 1] * plus[(t - k) % 8]
            b = b + coef[k - 1] * minus[(t + k) % 8]
        a = a + jnp.where(zero, 0.125 * (total_m - minus[t]), 0.0)
        b = jnp.where(zero, -0.25 * (total_p - plus[t]), b)
        out[72 * t : 72 * t + 36, :] = a
        out[72 * t + 36 : 72 * t + 72, :] = b
    for k, o in enumerate((o0, o1, o2, o3, o4, o5, o6, o7)):
        o[...] = out[pl.ds(pl.multiple_of(BLOCK * lax.rem(zc + k, 8), 8), BLOCK)]


def spread_groups(v, gi):
    level = [v]
    for width in (4, 2, 1):
        bit = (gi // width) % 2
        out = []
        for a in level:
            if width == 4:
                rolled = pltpu.roll(a, 64, 1)
            else:
                up = pltpu.roll(a, 16 * width, 1)
                down = pltpu.roll(a, 128 - 16 * width, 1)
                rolled = jnp.where(bit == 0, down, up)
            out.append(jnp.where(bit == 0, a, rolled))
            out.append(jnp.where(bit == 0, rolled, a))
        level = out
    return level


def backward_kernel(
    idx, r0, r1, r2, r3, r4, r5, r6, r7, before, after, own, wxth, wxtl, qts, wat, wbt, o0, o1, o2, o3, ds, gs, ab
):
    yc = idx[1]
    gather_z(idx[0], (r0, r1, r2, r3, r4, r5, r6, r7), ab)
    gi = lax.broadcasted_iota(jnp.int32, (EXTENT, 128), 1) // 16

    def along_z(m, carry):
        ta = jnp.concatenate([ab[pl.ds(m * 6 + i, 8, stride=72), :] for i in range(6)], axis=0)
        tb = jnp.concatenate([ab[pl.ds(36 + m * 6 + i, 8, stride=72), :] for i in range(6)], axis=0)
        las = spread_groups(ta, gi)
        lbs = spread_groups(tb, gi)
        place = pl.multiple_of(BLOCK + 48 * m, 8)
        prior = -12.0 * before[pl.ds(place, 48)]
        later = -12.0 * after[pl.ds(place, 48)]
        u = []
        for g in range(8):
            k = m * 8 + g
            v = own[k] + las[g] * wat[k] + lbs[g] * wbt[k]
            shift = ((7 - g) * 16) % 128
            edge = jnp.where(gi == 0, pltpu.roll(prior, (-g * 16) % 128, 1) if g else prior, 0.0)
            edge = jnp.where(gi == 7, pltpu.roll(later, shift, 1) if shift else later, edge)
            u.append(v + edge)
            if g % 2 == 1:
                pair = dot(qts[...], stack_of(jnp.concatenate(u, axis=1)), 1, 0)
                ds[k - 1] = pair[:, 0:128]
                ds[k] = pair[:, 128:256]
                u = []
        return carry

    lax.fori_loop(0, 6, along_z, 0)

    def along_x(j, carry):
        halves = []
        for half in range(2):
            place = pl.multiple_of(8 * (2 * j + half), 8)
            halves.append(ds[:, pl.ds(place, 8), :].reshape(384, 128))
        dh, dl = split_value(jnp.concatenate(halves, axis=1))
        wh = wxth[...]
        o = dot(wh, dh, 1, 0) + dot(wh, dl, 1, 0) + dot(wxtl[...], dh, 1, 0)
        for half in range(2):
            t = jnp.transpose(o[:, 128 * half : 128 * half + 128])
            for n in range(8):
                for f in range(2):
                    place = PLANE * n + 384 * (2 * j + half)
                    gs[f, :, pl.ds(pl.multiple_of(place, 128), 384)] = t[16 * n + 8 * f : 16 * n + 8 * f + 8]
        return carry

    lax.fori_loop(0, 3, along_x, 0)
    for k, out in enumerate((o0, o1, o2, o3)):
        yd = lax.rem(yc + k, 4)
        off = pl.multiple_of(yd * SITES + PLANE - 128, 128)
        off_extra = pl.multiple_of(yd * SITES + lax.rem(yd, 2) * 1152, 128)
        for f in range(2):
            out[f, :, 0:WIDE] = pltpu.roll(gs[f, :, pl.ds(off, WINDOW)], WIDE + 48, 1)[:, 0:WIDE]
            out[f, :, WIDE:WINDOW] = gs[f, :, pl.ds(off_extra, 128)]


def rotate_kernel(idx, r0, r1, r2, r3, theta, links, out, stats, sm, ex, gs, fix, deficit):
    step = pl.program_id(0)
    yc = idx[1]
    even = (yc % 2) == 0
    lane = lax.broadcasted_iota(jnp.int32, (8, 128), 1)

    @pl.when(step == 0)
    def _():
        rotations_of((r0, r1, r2, r3), yc, sm, ex, gs, fix)
        deficit[...] = jnp.zeros((8, 128), f32)

    xlast = (lax.broadcasted_iota(jnp.int32, (8, 384), 1) % EXTENT) == EXTENT - 1
    products(step, even, lane, xlast, links, out, gs, fix, deficit)

    @pl.when(step == 8)
    def _():
        row = lax.broadcasted_iota(jnp.int32, (8, 128), 0)
        line = jnp.sum(
            jnp.where(row == lane, jnp.sum(deficit[...], axis=1, keepdims=True), 0.0), axis=0, keepdims=True
        )
        total = jnp.sum(jnp.sum(theta[...], axis=1, keepdims=True), axis=0, keepdims=True)
        line = jnp.where(lane[0:1] == 8, total, line)
        stats[...] = jnp.broadcast_to(line, (32, 128))


def rotations_of(received, yc, sm, ex, gs, fix):
    for k, r in enumerate(received):
        c0 = 2 * lax.rem(yc - k + 4, 4)
        for f in range(2):
            sm[c0 + f] = r[f, :, 0:WIDE]
            ex[c0 + f] = r[f, :, WIDE : WIDE + 128]

    def store_rotation(load, store):
        g0, g1 = rotation_of([load(c) for c in range(8)])
        g2 = cross_conj(g0, g1)
        for i, g in enumerate((g0, g1, g2)):
            for c in range(3):
                for p in range(2):
                    store(6 * i + 2 * c + p, g[c][p])

    def rotations(q, carry):
        off = pl.multiple_of(q * 384, 128)

        def store(n, v):
            gs[n, :, pl.ds(off, 384)] = v

        store_rotation(lambda c: sm[c, :, pl.ds(off, 384)], store)
        return carry

    lax.fori_loop(0, 15, rotations, 0)

    def store_fix(n, v):
        fix[0, n] = v

    store_rotation(lambda c: ex[c], store_fix)
    for n in range(18):
        fix[1, n] = pltpu.roll(gs[n, :, 0:128], 80, 1)


def products(q, even, lane, xlast, links, out, gs, fix, deficit):
    off = pl.multiple_of(q * 384, 128)
    far = pl.multiple_of(q * 384 + PLANE, 128)
    from_fix = ((q == 0) & even) | ((q == 3) & jnp.logical_not(even)) | ((q == 6) & even)
    which = jnp.where(q == 6, 1, 0)
    head = (lane < 48) & from_fix

    def here(n):
        return gs[n, :, pl.ds(off, 384)]

    def ahead_x(n):
        v = here(n)
        return jnp.where(xlast, pltpu.roll(v, 47, 1), pltpu.roll(v, 383, 1))

    def ahead_y(n):
        return gs[n, :, pl.ds(far, 384)]

    def ahead_z(n):
        v = pltpu.roll(gs[n, :, pl.ds(off, 512)], 512 - 48, 1)[:, 0:384]
        return jnp.concatenate([jnp.where(head, fix[which, n], v[:, 0:128]), v[:, 128:384]], axis=1)

    def matrix(load):
        return [[(load(6 * i + 2 * c), load(6 * i + 2 * c + 1)) for c in range(3)] for i in range(3)]

    g = matrix(here)
    acc = jnp.zeros((8, 384), f32)
    for d, ahead in enumerate((ahead_x, ahead_y, ahead_z)):
        u0, u1 = two_rows_of(lambda n: links[12 * d + n, :, pl.ds(off, 384)])
        u = [u0, u1, cross_conj(u0, u1)]
        h = matrix(ahead)
        rows_out = []
        for i in range(2):
            t = []
            for j in range(3):
                v = cmul(g[i][0], u[0][j])
                for k in (1, 2):
                    v = cadd(v, cmul(g[i][k], u[k][j]))
                t.append(v)
            line = []
            for j in range(3):
                v = cmul_conj(t[0], h[j][0])
                for k in (1, 2):
                    v = cadd(v, cmul_conj(t[k], h[j][k]))
                line.append(v)
                out[12 * d + 6 * i + 2 * j] = v[0]
                out[12 * d + 6 * i + 2 * j + 1] = v[1]
            rows_out.append(line)
        a, b = rows_out
        corner = (a[0][0] * b[1][0] - a[0][1] * b[1][1]) - (a[1][0] * b[0][0] - a[1][1] * b[0][1])
        acc = acc + (3.0 - a[0][0] - b[1][0] - corner)
    deficit[...] += acc[:, 0:128] + acc[:, 128:256] + acc[:, 256:384]


def shape(*dims):
    return jax.ShapeDtypeStruct(dims, f32)


def call(kernel, outs, scalars, scratch=()):
    def run(*args):
        vm = pl.BlockSpec(memory_space=pltpu.VMEM)
        sm = pl.BlockSpec(memory_space=pltpu.SMEM)
        return pl.pallas_call(
            kernel,
            in_specs=[sm] * scalars + [vm] * (len(args) - scalars),
            out_specs=[vm] * len(outs),
            out_shape=list(outs),
            scratch_shapes=list(scratch),
            compiler_params=pltpu.CompilerParams(vmem_limit_bytes=24 * 1024 * 1024),
        )(*args)

    return run


def exchange_y(pieces):
    return [pieces[0]] + [from_behind(pieces[k], "space_1", k) for k in (1, 2, 3)]


def exchange_z(blocks):
    return [blocks[0]] + [from_behind(blocks[k], "space_0", k) for k in range(1, 8)]


def body(links):
    zc = lax.axis_index("space_0")
    yc = lax.axis_index("space_1")
    idx = jnp.stack([zc, yc]).astype(jnp.int32)
    px = jnp.asarray(PX)
    flat = links.transpose(1, 2, 3, 4, 0, 5).reshape(36, SLICES, SITES)
    window = shape(2, 8, WINDOW)
    modes = shape(48, 48, 128)
    packed = shape(6, 48, 128)
    (hs,) = call(project_kernel, [shape(24, 8, SITES)], 0)(flat)
    pieces = []
    for k in range(4):
        piece = functools.partial(gradient_kernel, k)
        (piece,) = call(piece, [window], 1, [pltpu.VMEM((8, SITES + 128), f32)])(idx, hs)
        pieces.append(piece)
    r = exchange_y(pieces)
    lam, kap = call(decay_kernel, [modes] * 2, 1)(px, jnp.asarray(PZ), hs)
    square = jax.ShapeDtypeStruct((384, 384), bf16)
    wxh, wxl, wxth, wxtl = call(matrix_kernel, [square] * 4, 0)(
        jnp.asarray(Q_HI), jnp.asarray(Q_LO), jnp.asarray(QT_HI), jnp.asarray(QT_LO), hs
    )
    block = shape(BLOCK, 128)
    long_block = shape(BLOCK + 288, 128)
    *blocks, own, e1, e6, theta = call(
        forward_kernel,
        [block, long_block] + [block] * 5 + [long_block, modes, packed, packed, shape(8, 128)],
        1,
        [
            pltpu.VMEM((2, 8, GROUP), f32),
            pltpu.VMEM((48, 48, 128), f32),
            pltpu.VMEM((6, 8, 128), f32),
            pltpu.VMEM((576, 128), f32),
        ],
    )(idx, *r, wxh, wxl, jnp.asarray(Q_STACK), lam, kap)
    blocks = exchange_z(blocks)
    before, after = blocks[1], blocks[7]
    *amps, theta = call(
        solve_kernel, [block] * 8 + [shape(8, 128)], 1, [pltpu.VMEM((576, 128), f32)] * 2
    )(idx, *blocks, jnp.asarray(PSUM), e1, e6, theta)
    wa, wb = call(weight_kernel, [modes] * 2, 1)(px, jnp.asarray(PZ), amps[0])
    theta = theta + from_behind(theta, "tm_1", 1)
    theta = theta + sum(from_behind(theta, "tm_0", k) for k in (1, 2, 3))
    amps = exchange_z(amps)
    windows = call(
        backward_kernel,
        [window] * 4,
        1,
        [pltpu.VMEM((48, 48, 128), f32), pltpu.VMEM((2, 8, GROUP), f32), pltpu.VMEM((576, 128), f32)],
    )(
        idx, *amps, before, after, own, wxth, wxtl, jnp.asarray(QT_STACK), wa, wb,
    )
    r = exchange_y(windows)
    again, _ = lax.optimization_barrier((links, windows[1]))
    flat = again.transpose(1, 2, 3, 4, 0, 5).reshape(36, SLICES, SITES)
    vm = pl.BlockSpec(memory_space=pltpu.VMEM)
    new_flat, stats = pl.pallas_call(
        rotate_kernel,
        grid=(9,),
        in_specs=[pl.BlockSpec(memory_space=pltpu.SMEM)] + [vm] * 6,
        out_specs=[pl.BlockSpec((36, 8, 384), lambda q: (0, 0, q)), pl.BlockSpec((32, 128), lambda q: (0, 0))],
        out_shape=[pltpu.HBM((36, 8, SITES), f32), shape(32, 128)],
        scratch_shapes=[
            pltpu.VMEM((8, 8, WIDE), f32),
            pltpu.VMEM((8, 8, 128), f32),
            pltpu.VMEM((18, 8, WIDE), f32),
            pltpu.VMEM((2, 18, 8, 128), f32),
            pltpu.VMEM((8, 128), f32),
        ],
        compiler_params=pltpu.CompilerParams(vmem_limit_bytes=24 * 1024 * 1024),
    )(idx, *r, theta, flat)
    new_links = new_flat.reshape(3, 2, 3, 2, SLICES, SITES).transpose(4, 0, 1, 2, 3, 5)
    both = jnp.sum(lax.all_to_all(stats, SPACE, split_axis=0, concat_axis=0, tiled=True), axis=0)
    theta = both[8] / (SLICES * 8 * EXTENT**3)
    deficit = both[:8] / EXTENT**3
    return (new_links, theta, deficit)


def solution(mesh):
    torus = Mesh(mesh.devices.reshape(4, 2, 8, 4), ("tm_0", "tm_1", "space_0", "space_1"))
    in_specs = (P(TM, None, None, None, None, SPACE),)
    out_specs = (P(TM, None, None, None, None, SPACE), P(), P(TM))
    return jax.shard_map(body, mesh=torus, in_specs=in_specs, out_specs=out_specs, check_vma=False)
```

```python
import functools
import math

import jax
import jax.numpy as jnp
import numpy as np
from jax import lax
from jax.experimental import pallas as pl
from jax.experimental.pallas import tpu as pltpu
from jax.sharding import Mesh
from jax.sharding import PartitionSpec as P

EXTENT = 48
SPACE = ("space_0", "space_1")
TM = ("tm_0", "tm_1")
TM_SPACE = ("tm_0", "tm_1", "space_0", "space_1")
SLICES = 8
ROWS = 72
SITES = ROWS * EXTENT
PLANE = EXTENT * EXTENT
WIDE = SITES + PLANE
WINDOW = WIDE + 128
BLOCK = 72
GROUP = 8 * PLANE

root_three = math.sqrt(3.0)
step_size = 0.08
f32 = jnp.float32
bf16 = jnp.bfloat16


def from_behind(block, axis, distance):
    n = lax.axis_size(axis)
    return lax.ppermute(block, axis, [((i - distance) % n, i) for i in range(n)])


def basis():
    k = np.arange(25)[:, None]
    x = np.arange(EXTENT)[None, :]
    cos = np.cos(2 * np.pi * k * x / EXTENT) * math.sqrt(2 / EXTENT)
    cos[0] /= math.sqrt(2)
    cos[24] /= math.sqrt(2)
    sin = np.sin(2 * np.pi * k * x / EXTENT) * math.sqrt(2 / EXTENT)
    return np.concatenate([cos, sin[1:24]], axis=0)


def wave_terms():
    k = np.concatenate([np.arange(25), np.arange(1, 24)])
    return 4 * np.sin(np.pi * k / EXTENT) ** 2


def split_bf16(a):
    a = np.asarray(a, np.float32)
    hi = a.astype(jnp.bfloat16)
    lo = (a - hi.astype(np.float32)).astype(jnp.bfloat16)
    return hi, lo


Q = basis()
P2 = wave_terms()
Q_HI, Q_LO = split_bf16(Q)
QT_HI, QT_LO = split_bf16(Q.T)
Q_STACK = np.concatenate([Q_HI, Q_HI, Q_LO], axis=1)
QT_STACK = np.concatenate([QT_HI, QT_HI, QT_LO], axis=1)
PZ = np.repeat(P2[:, None], 128, axis=1).astype(np.float32)
PX = P2.astype(np.float32)
PXM = np.repeat(np.repeat(P2.reshape(6, 1, 8), 6, axis=1).reshape(36, 8), 16, axis=1)
PZM = np.repeat(np.tile(P2.reshape(6, 8).T[:, None, :], (1, 6, 1)).reshape(8, 36, 1), 128, axis=2)
PSUM = (PXM[None] + PZM).astype(np.float32)


def zero_green(distance):
    d = np.arange(EXTENT)
    mean = np.mean(d * d / 96 - d / 2)
    return float(12 * (distance * distance / 96 - distance / 2 - mean))


def cmul(p, q):
    return (p[0] * q[0] - p[1] * q[1], p[0] * q[1] + p[1] * q[0])


def cmul_conj(p, q):
    return (p[0] * q[0] + p[1] * q[1], p[1] * q[0] - p[0] * q[1])


def cadd(p, q):
    return (p[0] + q[0], p[1] + q[1])


def csub(p, q):
    return (p[0] - q[0], p[1] - q[1])


def cross_conj(a, b):
    out = []
    for k in range(3):
        p = cmul(a[(k + 1) % 3], b[(k + 2) % 3])
        q = cmul(a[(k + 2) % 3], b[(k + 1) % 3])
        out.append((p[0] - q[0], q[1] - p[1]))
    return out


def algebra_of(u0, u1):
    u2 = cross_conj(u0, u1)
    return [
        u0[1][1] + u1[0][1],
        u0[1][0] - u1[0][0],
        u0[0][1] - u1[1][1],
        u0[2][1] + u2[0][1],
        u0[2][0] - u2[0][0],
        u1[2][1] + u2[1][1],
        u1[2][0] - u2[1][0],
        (u0[0][1] + u1[1][1] - 2.0 * u2[2][1]) * (1.0 / root_three),
    ]


def rotation_of(a):
    half = 0.5 * step_size
    a = [half * v for v in a]
    e = a[7] * (1.0 / root_three)
    diag = [a[2] + e, e - a[2], -2.0 * e]
    zero = jnp.zeros_like(a[0])
    x = [
        [(zero, diag[0]), (a[1], a[0]), (a[4], a[3])],
        [(-a[1], a[0]), (zero, diag[1]), (a[6], a[5])],
        [(-a[4], a[3]), (-a[6], a[5]), (zero, diag[2])],
    ]

    def entry(i, j):
        total = None
        for k in range(3):
            p, q = x[i][k], x[k][j]
            if i == k and k == j:
                term = (-p[1] * q[1], None)
            elif i == k:
                term = (-p[1] * q[1], p[1] * q[0])
            elif k == j:
                term = (-p[1] * q[1], p[0] * q[1])
            else:
                term = cmul(p, q)
            if total is None:
                total = term
            else:
                re = total[0] + term[0]
                if total[1] is None:
                    im = term[1]
                elif term[1] is None:
                    im = total[1]
                else:
                    im = total[1] + term[1]
                total = (re, im)
        re = 0.5 * total[0] + x[i][j][0] if i != j else 0.5 * total[0] + 1.0
        im = 0.5 * total[1] + x[i][j][1]
        return (re, im)

    m0 = [entry(0, j) for j in range(3)]
    m1 = [entry(1, j) for j in range(3)]
    inv = lax.rsqrt(sum(p[0] * p[0] + p[1] * p[1] for p in m0))
    r0 = [(p[0] * inv, p[1] * inv) for p in m0]
    corr = cmul_conj(m1[0], r0[0])
    for k in (1, 2):
        corr = cadd(corr, cmul_conj(m1[k], r0[k]))
    w = [csub(m1[k], cmul(corr, r0[k])) for k in range(3)]
    inv = lax.rsqrt(sum(p[0] * p[0] + p[1] * p[1] for p in w))
    r1 = [(p[0] * inv, p[1] * inv) for p in w]
    return r0, r1


def two_rows_of(load):
    u0 = [(load(2 * c), load(2 * c + 1)) for c in range(3)]
    u1 = [(load(6 + 2 * c), load(6 + 2 * c + 1)) for c in range(3)]
    return u0, u1


def project_kernel(links, hs):
    def project(q, carry):
        off = pl.multiple_of(q * 384, 128)
        for d in range(3):
            u0, u1 = two_rows_of(lambda n: links[12 * d + n, :, pl.ds(off, 384)])
            for c, h in enumerate(algebra_of(u0, u1)):
                hs[d * 8 + c, :, pl.ds(off, 384)] = h
        return carry

    lax.fori_loop(0, 9, project, 0)


def gradient_kernel(shift, idx, hs, out, zb):
    yc = idx[1]
    even = (yc % 2) == 0
    width = SITES + 128
    xzero = (lax.broadcasted_iota(jnp.int32, (8, SITES), 1) % EXTENT) == 0
    lane = lax.broadcasted_iota(jnp.int32, (8, 128), 1)
    first = lane < 48
    second = (lane >= 48) & (lane < 96)
    zeros = jnp.zeros((8, 128), f32)

    def combine(f, carry):
        c = 2 * lax.rem(yc + shift, 4) + f
        hx = hs[c]
        hy = jnp.concatenate([hs[8 + c], zeros], axis=1)
        hz = hs[16 + c]
        zb[...] = pltpu.roll(jnp.concatenate([hz, zeros], axis=1), 48, 1)
        head = zb[:, 0:128]
        zb[:, 0:128] = jnp.where(second & even, pltpu.roll(hz[:, 2304:2432], 48, 1), head)
        zb[:, 2304:2432] = jnp.where(second & even, 0.0, zb[:, 2304:2432])
        zb[:, 1152:1280] = jnp.where(second & jnp.logical_not(even), 0.0, zb[:, 1152:1280])
        bx = jnp.where(xzero, pltpu.roll(hx, SITES - 47, 1), pltpu.roll(hx, 1, 1))
        near = (bx - hx) - hz - hs[8 + c]
        p = jnp.concatenate([near, zeros], axis=1) + zb[...]
        p = pltpu.roll(p, 80, 1)
        ha = pltpu.roll(hy, 80, 1)
        out[f, :, 0:PLANE] = p[:, 0:PLANE]
        out[f, :, PLANE:width] = p[:, PLANE:width] + ha[:, 0 : width - PLANE]
        out[f, :, width:WINDOW] = ha[:, width - PLANE : width]
        wrap = jnp.where(even, hz[:, 0:128], hz[:, 1152:1280])
        out[f, :, WIDE:WINDOW] += pltpu.roll(jnp.where(first, wrap, 0.0), 80, 1)
        return carry

    for f in range(2):
        combine(f, 0)


def lambda_of(m):
    s = jnp.sqrt(m + 0.25 * m * m)
    return 1.0 / (1.0 + 0.5 * m + s), s


def split_value(a):
    hi = a.astype(bf16)
    return hi, (a - hi.astype(f32)).astype(bf16)


def dot(a, b, ca, cb):
    return lax.dot_general(a, b, (((ca,), (cb,)), ((), ())), preferred_element_type=f32)


def stack_of(a):
    hi, lo = split_value(a)
    return jnp.concatenate([hi, lo, hi], axis=0)


def decay_kernel(px, pz, after, lam_out, kap_out):
    def one(k, carry):
        lam, s = lambda_of(px[k] + pz[...])
        lam_out[k] = lam
        kap_out[k] = 6.0 / s
        return carry

    lax.fori_loop(0, EXTENT, one, 0)


def weight_kernel(px, pz, after, wa_out, wb_out):
    gi = lax.broadcasted_iota(jnp.int32, (EXTENT, 128), 1) // 16
    row = lax.broadcasted_iota(jnp.int32, (EXTENT, 128), 0)
    gr = 7 - gi

    def one(k, carry):
        lam, s = lambda_of(px[k] + pz[...])
        lam2 = lam * lam
        lam4 = lam2 * lam2
        wa = jnp.where(gi % 2 == 1, lam, 1.0) * jnp.where((gi // 2) % 2 == 1, lam2, 1.0)
        wa_out[k] = wa * jnp.where(gi >= 4, lam4, 1.0)
        wb = jnp.where(gr % 2 == 1, lam, 1.0) * jnp.where((gr // 2) % 2 == 1, lam2, 1.0)
        wb_out[k] = jnp.where((row == 0) & (k == 0), gi.astype(f32), wb * jnp.where(gr >= 4, lam4, 1.0))
        return carry

    lax.fori_loop(0, EXTENT, one, 0)


def matrix_kernel(qh, ql, qth, qtl, after, wxh, wxl, wxth, wxtl):
    def where_one(cond):
        return jnp.where(cond, 1.0, 0.0).astype(bf16)

    tall = lax.broadcasted_iota(jnp.int32, (384, EXTENT), 0)
    narrow = lax.broadcasted_iota(jnp.int32, (384, EXTENT), 1)
    wide = lax.broadcasted_iota(jnp.int32, (EXTENT, 384), 1)
    short = lax.broadcasted_iota(jnp.int32, (EXTENT, 384), 0)
    row = lax.broadcasted_iota(jnp.int32, (384, 384), 0)
    col = lax.broadcasted_iota(jnp.int32, (384, 384), 1)
    mask = (row % 8) == (col // EXTENT)
    mask_t = (row // EXTENT) == (col % 8)
    from_k = where_one(tall // 8 == narrow)
    to_x = where_one(wide % EXTENT == short)
    from_x = where_one(tall % EXTENT == narrow)
    to_k = where_one(wide // 8 == short)
    for q, out in ((qh, wxh), (ql, wxl)):
        a = dot(from_k, q[...], 1, 0).astype(bf16)
        out[...] = jnp.where(mask, dot(a, to_x, 1, 0), 0.0).astype(bf16)
    for q, out in ((qth, wxth), (qtl, wxtl)):
        a = dot(from_x, q[...], 1, 0).astype(bf16)
        out[...] = jnp.where(mask_t, dot(a, to_k, 1, 0), 0.0).astype(bf16)


def forward_kernel(
    idx, r0, r1, r2, r3, wxh, wxl, qs, lamt, kapt, m0, m1, m2, m3, m4, m5, m6, m7, own, e1o, e6o, theta, gs, ds, es, sout
):
    zc = idx[0]
    yc = idx[1]
    lane = lax.broadcasted_iota(jnp.int32, (8, 128), 1)
    gs[...] = jnp.zeros((2, 8, GROUP), f32)
    for k, r in enumerate((r0, r1, r2, r3)):
        yd = lax.rem(yc - k + 4, 4)
        off = pl.multiple_of(yd * SITES + PLANE - 128, 128)
        off_end = pl.multiple_of(yd * SITES + PLANE - 128 + WIDE, 128)
        off_wrap = pl.multiple_of(yd * SITES + lax.rem(yd, 2) * 1152, 128)
        for f in range(2):
            gs[f, :, pl.ds(off, WIDE)] += r[f, :, 0:WIDE]
            tail = r[f, :, WIDE:WINDOW]
            gs[f, :, pl.ds(off_end, 128)] += jnp.where(lane < 80, tail, 0.0)
            gs[f, :, pl.ds(off_wrap, 128)] += jnp.where(lane < 48, pltpu.roll(tail, 48, 1), 0.0)

    def along_x(j, carry):
        pieces = []
        for half in range(2):
            for n in range(8):
                for f in range(2):
                    place = PLANE * n + 384 * (2 * j + half)
                    pieces.append(gs[f, :, pl.ds(pl.multiple_of(place, 128), 384)])
        bh, bl = split_value(jnp.concatenate(pieces, axis=0))
        wh = wxh[...]
        out = dot(wh, bh, 1, 1) + dot(wh, bl, 1, 1) + dot(wxl[...], bh, 1, 1)
        for half in range(2):
            place = pl.multiple_of(8 * (2 * j + half), 8)
            ds[:, pl.ds(place, 8), :] = out[:, 128 * half : 128 * half + 128].reshape(EXTENT, 8, 128)
        return carry

    lax.fori_loop(0, 3, along_x, 0)

    gi = lax.broadcasted_iota(jnp.int32, (EXTENT, 128), 1) // 16

    def along_z(m, squares):
        packs = [jnp.zeros((EXTENT, 128), f32) for _ in range(6)]
        pair = None
        for g in range(8):
            k = m * 8 + g
            if g % 2 == 0:
                pair = dot(qs[...], stack_of(jnp.concatenate([ds[k], ds[k + 1]], axis=1)), 1, 0)
            e = pair[:, 128 * (g % 2) : 128 * (g % 2) + 128]
            if g == 0:
                es[m] = e[0:8]
            lam = lamt[k]
            lam2 = lam * lam
            lam4 = lam2 * lam2
            up = e + jnp.where(gi >= 1, lam, 0.0) * pltpu.roll(e, 16, 1)
            up = up + jnp.where(gi >= 2, lam2, 0.0) * pltpu.roll(up, 32, 1)
            up = up + jnp.where(gi >= 4, lam4, 0.0) * pltpu.roll(up, 64, 1)
            down = e + jnp.where(gi <= 6, lam, 0.0) * pltpu.roll(e, 112, 1)
            down = down + jnp.where(gi <= 5, lam2, 0.0) * pltpu.roll(down, 96, 1)
            down = down + jnp.where(gi <= 3, lam4, 0.0) * pltpu.roll(down, 64, 1)
            own[k] = kapt[k] * (up + down - e)
            squares = squares + sum(e[8 * i : 8 * i + 8] * e[8 * i : 8 * i + 8] for i in range(6))
            for n, (v, source) in enumerate(((up, 7), (down, 0), (e, 7), (e, 0), (e, 1), (e, 6))):
                shift = ((g - source) * 16) % 128
                packs[n] = jnp.where(gi == g, pltpu.roll(v, shift, 1) if shift else v, packs[n])
        for i in range(6):
            sout[pl.ds(m * 6 + i, 8, stride=72), :] = packs[0][8 * i : 8 * i + 8]
            sout[pl.ds(36 + m * 6 + i, 8, stride=72), :] = packs[1][8 * i : 8 * i + 8]
        m1[pl.ds(pl.multiple_of(BLOCK + 48 * m, 8), 48)] = packs[2]
        m7[pl.ds(pl.multiple_of(BLOCK + 48 * m, 8), 48)] = packs[3]
        e1o[m] = packs[4]
        e6o[m] = packs[5]
        return squares

    squares = lax.fori_loop(0, 6, along_z, jnp.zeros((8, 128), f32))

    e0 = es[0]
    gt = lane // 16
    row = lax.broadcasted_iota(jnp.int32, (8, 128), 0)
    total = zero_green(0) * e0
    for n in range(1, 8):
        weight = jnp.where(gt >= n, zero_green(n), zero_green(8 - n))
        total = total + weight * pltpu.roll(e0, 16 * n, 1)
    own[0, 0:8, :] = jnp.where(row == 0, total, own[0, 0:8, :])
    theta[...] = jnp.where((gt >= 2) & (gt <= 5), squares, 0.0)
    yf = gt.astype(f32)

    def over_groups(v):
        for n in (16, 32, 64):
            v = v + pltpu.roll(v, n, 1)
        return v

    first = over_groups(yf * e0)
    second = over_groups(yf * yf * e0)
    here = (row == 0) & (gt == 0)
    sout[0:8, :] = jnp.where(here, first, sout[0:8, :])
    sout[36:44, :] = jnp.where(here, second, sout[36:44, :])
    for k, o in enumerate((m0, m1, m2, m3, m4, m5, m6, m7)):
        o[0:BLOCK] = sout[pl.ds(pl.multiple_of(BLOCK * lax.rem(zc + k, 8), 8), BLOCK)]


def gather_z(zc, blocks, s):
    for k, r in enumerate(blocks):
        s[pl.ds(pl.multiple_of(BLOCK * lax.rem(zc - k + 8, 8), 8), BLOCK)] = r[0:BLOCK]


def solve_kernel(
    idx, r0, r1, r2, r3, r4, r5, r6, r7, psum, e1, e6, theta_in, o0, o1, o2, o3, o4, o5, o6, o7, theta, s, out
):
    zc = idx[0]
    gather_z(zc, (r0, r1, r2, r3, r4, r5, r6, r7), s)
    squares = theta_in[...]
    for m in range(6):
        for i in range(6):
            place = BLOCK + 48 * m + 8 * i
            plane_first = e1[m, 8 * i : 8 * i + 8] + r1[place : place + 8]
            plane_last = e6[m, 8 * i : 8 * i + 8] + r7[place : place + 8]
            squares = squares + plane_first * plane_first + plane_last * plane_last
    theta[...] = squares
    lam, root = lambda_of(psum[zc])
    lam2 = lam * lam
    lam6 = lam2 * lam2 * lam2
    lam12 = lam6 * lam6
    lam24 = lam12 * lam12
    row = lax.broadcasted_iota(jnp.int32, (36, 128), 0)
    lane = lax.broadcasted_iota(jnp.int32, (36, 128), 1)
    zero = (row == 0) & (lane < 16) & (zc == 0)
    kappa = 6.0 / root / (1.0 - lam24 * lam24)
    coef = []
    power = 1.0 + 0.5 * psum[zc] + root
    for k in range(1, 9):
        coef.append(kappa * power)
        power = power * lam6
    plus = [s[72 * n : 72 * n + 36, :] for n in range(8)]
    minus = [s[72 * n + 36 : 72 * n + 72, :] for n in range(8)]
    total_p = sum(plus)
    total_m = sum(minus)
    coef_a = [jnp.where(zero, 12.0 * (0.5 - k / 8.0) if k < 8 else 0.0, coef[k - 1]) for k in range(1, 9)]
    for t in range(8):
        a = coef_a[0] * plus[(t - 1) % 8]
        b = coef[0] * minus[(t + 1) % 8]
        for k in range(2, 9):
            a = a + coef_a[k - 1] * plus[(t - k) % 8]
            b = b + coef[k - 1] * minus[(t + k) % 8]
        a = a + jnp.where(zero, 0.125 * (total_m - minus[t]), 0.0)
        b = jnp.where(zero, -0.25 * (total_p - plus[t]), b)
        out[72 * t : 72 * t + 36, :] = a
        out[72 * t + 36 : 72 * t + 72, :] = b
    for k, o in enumerate((o0, o1, o2, o3, o4, o5, o6, o7)):
        o[...] = out[pl.ds(pl.multiple_of(BLOCK * lax.rem(zc + k, 8), 8), BLOCK)]


def spread_groups(v, gi):
    level = [v]
    for width in (4, 2, 1):
        bit = (gi // width) % 2
        out = []
        for a in level:
            if width == 4:
                rolled = pltpu.roll(a, 64, 1)
            else:
                up = pltpu.roll(a, 16 * width, 1)
                down = pltpu.roll(a, 128 - 16 * width, 1)
                rolled = jnp.where(bit == 0, down, up)
            out.append(jnp.where(bit == 0, a, rolled))
            out.append(jnp.where(bit == 0, rolled, a))
        level = out
    return level


def backward_kernel(
    idx, r0, r1, r2, r3, r4, r5, r6, r7, before, after, own, wxth, wxtl, qts, wat, wbt, o0, o1, o2, o3, ds, gs, ab
):
    yc = idx[1]
    gather_z(idx[0], (r0, r1, r2, r3, r4, r5, r6, r7), ab)
    gi = lax.broadcasted_iota(jnp.int32, (EXTENT, 128), 1) // 16

    def along_z(m, carry):
        ta = jnp.concatenate([ab[pl.ds(m * 6 + i, 8, stride=72), :] for i in range(6)], axis=0)
        tb = jnp.concatenate([ab[pl.ds(36 + m * 6 + i, 8, stride=72), :] for i in range(6)], axis=0)
        las = spread_groups(ta, gi)
        lbs = spread_groups(tb, gi)
        place = pl.multiple_of(BLOCK + 48 * m, 8)
        prior = -12.0 * before[pl.ds(place, 48)]
        later = -12.0 * after[pl.ds(place, 48)]
        u = []
        for g in range(8):
            k = m * 8 + g
            v = own[k] + las[g] * wat[k] + lbs[g] * wbt[k]
            shift = ((7 - g) * 16) % 128
            edge = jnp.where(gi == 0, pltpu.roll(prior, (-g * 16) % 128, 1) if g else prior, 0.0)
            edge = jnp.where(gi == 7, pltpu.roll(later, shift, 1) if shift else later, edge)
            u.append(v + edge)
            if g % 2 == 1:
                pair = dot(qts[...], stack_of(jnp.concatenate(u, axis=1)), 1, 0)
                ds[k - 1] = pair[:, 0:128]
                ds[k] = pair[:, 128:256]
                u = []
        return carry

    lax.fori_loop(0, 6, along_z, 0)

    def along_x(j, carry):
        halves = []
        for half in range(2):
            place = pl.multiple_of(8 * (2 * j + half), 8)
            halves.append(ds[:, pl.ds(place, 8), :].reshape(384, 128))
        dh, dl = split_value(jnp.concatenate(halves, axis=1))
        wh = wxth[...]
        o = dot(wh, dh, 1, 0) + dot(wh, dl, 1, 0) + dot(wxtl[...], dh, 1, 0)
        for half in range(2):
            t = jnp.transpose(o[:, 128 * half : 128 * half + 128])
            for n in range(8):
                for f in range(2):
                    place = PLANE * n + 384 * (2 * j + half)
                    gs[f, :, pl.ds(pl.multiple_of(place, 128), 384)] = t[16 * n + 8 * f : 16 * n + 8 * f + 8]
        return carry

    lax.fori_loop(0, 3, along_x, 0)
    for k, out in enumerate((o0, o1, o2, o3)):
        yd = lax.rem(yc + k, 4)
        off = pl.multiple_of(yd * SITES + PLANE - 128, 128)
        off_extra = pl.multiple_of(yd * SITES + lax.rem(yd, 2) * 1152, 128)
        for f in range(2):
            out[f, :, 0:WIDE] = pltpu.roll(gs[f, :, pl.ds(off, WINDOW)], WIDE + 48, 1)[:, 0:WIDE]
            out[f, :, WIDE:WINDOW] = gs[f, :, pl.ds(off_extra, 128)]


def rotate_kernel(idx, r0, r1, r2, r3, theta, links, out, stats, sm, ex, gs, fix, deficit):
    step = pl.program_id(0)
    yc = idx[1]
    even = (yc % 2) == 0
    lane = lax.broadcasted_iota(jnp.int32, (8, 128), 1)

    @pl.when(step == 0)
    def _():
        rotations_of((r0, r1, r2, r3), yc, sm, ex, gs, fix)
        deficit[...] = jnp.zeros((8, 128), f32)

    xlast = (lax.broadcasted_iota(jnp.int32, (8, 384), 1) % EXTENT) == EXTENT - 1

    def chunk(sub, carry):
        products(step * 3 + sub, sub, even, lane, xlast, links, out, gs, fix, deficit)
        return carry

    lax.fori_loop(0, 3, chunk, 0)

    @pl.when(step == 2)
    def _():
        row = lax.broadcasted_iota(jnp.int32, (8, 128), 0)
        line = jnp.sum(
            jnp.where(row == lane, jnp.sum(deficit[...], axis=1, keepdims=True), 0.0), axis=0, keepdims=True
        )
        total = jnp.sum(jnp.sum(theta[...], axis=1, keepdims=True), axis=0, keepdims=True)
        line = line * (1.0 / EXTENT**3)
        line = jnp.where(lane[0:1] == 8, total * (1.0 / (SLICES * 8 * EXTENT**3)), line)
        stats[...] = jnp.broadcast_to(line, (32, 128))


def rotations_of(received, yc, sm, ex, gs, fix):
    for k, r in enumerate(received):
        c0 = 2 * lax.rem(yc - k + 4, 4)
        for f in range(2):
            sm[c0 + f] = r[f, :, 0:WIDE]
            ex[c0 + f] = r[f, :, WIDE : WIDE + 128]

    def store_rotation(load, store):
        g0, g1 = rotation_of([load(c) for c in range(8)])
        g2 = cross_conj(g0, g1)
        for i, g in enumerate((g0, g1, g2)):
            for c in range(3):
                for p in range(2):
                    store(6 * i + 2 * c + p, g[c][p])

    def rotations(q, carry):
        off = pl.multiple_of(q * 384, 128)

        def store(n, v):
            gs[n, :, pl.ds(off, 384)] = v

        store_rotation(lambda c: sm[c, :, pl.ds(off, 384)], store)
        return carry

    lax.fori_loop(0, 15, rotations, 0)

    def store_fix(n, v):
        fix[0, n] = v

    store_rotation(lambda c: ex[c], store_fix)
    for n in range(18):
        fix[1, n] = pltpu.roll(gs[n, :, 0:128], 80, 1)


def products(q, sub, even, lane, xlast, links, out, gs, fix, deficit):
    local = pl.multiple_of(sub * 384, 128)
    off = pl.multiple_of(q * 384, 128)
    far = pl.multiple_of(q * 384 + PLANE, 128)
    from_fix = ((q == 0) & even) | ((q == 3) & jnp.logical_not(even)) | ((q == 6) & even)
    which = jnp.where(q == 6, 1, 0)
    head = (lane < 48) & from_fix

    def here(n):
        return gs[n, :, pl.ds(off, 384)]

    def ahead_x(n):
        v = here(n)
        return jnp.where(xlast, pltpu.roll(v, 47, 1), pltpu.roll(v, 383, 1))

    def ahead_y(n):
        return gs[n, :, pl.ds(far, 384)]

    def ahead_z(n):
        v = pltpu.roll(gs[n, :, pl.ds(off, 512)], 512 - 48, 1)[:, 0:384]
        return jnp.concatenate([jnp.where(head, fix[which, n], v[:, 0:128]), v[:, 128:384]], axis=1)

    def matrix(load):
        return [[(load(6 * i + 2 * c), load(6 * i + 2 * c + 1)) for c in range(3)] for i in range(3)]

    g = matrix(here)
    acc = jnp.zeros((8, 384), f32)
    for d, ahead in enumerate((ahead_x, ahead_y, ahead_z)):
        u0, u1 = two_rows_of(lambda n: links[12 * d + n, :, pl.ds(off, 384)])
        u = [u0, u1, cross_conj(u0, u1)]
        h = matrix(ahead)
        rows_out = []
        for i in range(2):
            t = []
            for j in range(3):
                v = cmul(g[i][0], u[0][j])
                for k in (1, 2):
                    v = cadd(v, cmul(g[i][k], u[k][j]))
                t.append(v)
            line = []
            for j in range(3):
                v = cmul_conj(t[0], h[j][0])
                for k in (1, 2):
                    v = cadd(v, cmul_conj(t[k], h[j][k]))
                line.append(v)
                out[12 * d + 6 * i + 2 * j, :, pl.ds(local, 384)] = v[0]
                out[12 * d + 6 * i + 2 * j + 1, :, pl.ds(local, 384)] = v[1]
            rows_out.append(line)
        a, b = rows_out
        corner = (a[0][0] * b[1][0] - a[0][1] * b[1][1]) - (a[1][0] * b[0][0] - a[1][1] * b[0][1])
        acc = acc + (3.0 - a[0][0] - b[1][0] - corner)
    deficit[...] += acc[:, 0:128] + acc[:, 128:256] + acc[:, 256:384]


def shape(*dims):
    return jax.ShapeDtypeStruct(dims, f32)


def call(kernel, outs, scalars, scratch=()):
    def run(*args):
        vm = pl.BlockSpec(memory_space=pltpu.VMEM)
        sm = pl.BlockSpec(memory_space=pltpu.SMEM)
        return pl.pallas_call(
            kernel,
            in_specs=[sm] * scalars + [vm] * (len(args) - scalars),
            out_specs=[vm] * len(outs),
            out_shape=list(outs),
            scratch_shapes=list(scratch),
            compiler_params=pltpu.CompilerParams(vmem_limit_bytes=24 * 1024 * 1024),
        )(*args)

    return run


def exchange_y(pieces):
    return [pieces[0]] + [from_behind(pieces[k], "space_1", k) for k in (1, 2, 3)]


def exchange_z(blocks):
    return [blocks[0]] + [from_behind(blocks[k], "space_0", k) for k in range(1, 8)]


def body(links):
    zc = lax.axis_index("space_0")
    yc = lax.axis_index("space_1")
    idx = jnp.stack([zc, yc]).astype(jnp.int32)
    px = jnp.asarray(PX)
    flat = links.transpose(1, 2, 3, 4, 0, 5).reshape(36, SLICES, SITES)
    window = shape(2, 8, WINDOW)
    modes = shape(48, 48, 128)
    packed = shape(6, 48, 128)
    (hs,) = call(project_kernel, [shape(24, 8, SITES)], 0)(flat)
    pieces = []
    for k in range(4):
        piece = functools.partial(gradient_kernel, k)
        (piece,) = call(piece, [window], 1, [pltpu.VMEM((8, SITES + 128), f32)])(idx, hs)
        pieces.append(piece)
    r = exchange_y(pieces)
    lam, kap = call(decay_kernel, [modes] * 2, 1)(px, jnp.asarray(PZ), hs)
    square = jax.ShapeDtypeStruct((384, 384), bf16)
    wxh, wxl, wxth, wxtl = call(matrix_kernel, [square] * 4, 0)(
        jnp.asarray(Q_HI), jnp.asarray(Q_LO), jnp.asarray(QT_HI), jnp.asarray(QT_LO), hs
    )
    block = shape(BLOCK, 128)
    long_block = shape(BLOCK + 288, 128)
    *blocks, own, e1, e6, theta = call(
        forward_kernel,
        [block, long_block] + [block] * 5 + [long_block, modes, packed, packed, shape(8, 128)],
        1,
        [
            pltpu.VMEM((2, 8, GROUP), f32),
            pltpu.VMEM((48, 48, 128), f32),
            pltpu.VMEM((6, 8, 128), f32),
            pltpu.VMEM((576, 128), f32),
        ],
    )(idx, *r, wxh, wxl, jnp.asarray(Q_STACK), lam, kap)
    blocks = exchange_z(blocks)
    before, after = blocks[1], blocks[7]
    *amps, theta = call(
        solve_kernel, [block] * 8 + [shape(8, 128)], 1, [pltpu.VMEM((576, 128), f32)] * 2
    )(idx, *blocks, jnp.asarray(PSUM), e1, e6, theta)
    wa, wb = call(weight_kernel, [modes] * 2, 1)(px, jnp.asarray(PZ), amps[0])
    theta = theta + from_behind(theta, "tm_1", 1)
    theta = theta + sum(from_behind(theta, "tm_0", k) for k in (1, 2, 3))
    amps = exchange_z(amps)
    windows = call(
        backward_kernel,
        [window] * 4,
        1,
        [pltpu.VMEM((48, 48, 128), f32), pltpu.VMEM((2, 8, GROUP), f32), pltpu.VMEM((576, 128), f32)],
    )(
        idx, *amps, before, after, own, wxth, wxtl, jnp.asarray(QT_STACK), wa, wb,
    )
    r = exchange_y(windows)
    again, _ = lax.optimization_barrier((links, windows[1]))
    flat = again.transpose(1, 2, 3, 4, 0, 5).reshape(36, SLICES, SITES)
    vm = pl.BlockSpec(memory_space=pltpu.VMEM)
    new_flat, stats = pl.pallas_call(
        rotate_kernel,
        grid=(3,),
        in_specs=[pl.BlockSpec(memory_space=pltpu.SMEM)] + [vm] * 6,
        out_specs=[pl.BlockSpec((36, 8, 1152), lambda q: (0, 0, q)), pl.BlockSpec((32, 128), lambda q: (0, 0))],
        out_shape=[pltpu.HBM((36, 8, SITES), f32), shape(32, 128)],
        scratch_shapes=[
            pltpu.VMEM((8, 8, WIDE), f32),
            pltpu.VMEM((8, 8, 128), f32),
            pltpu.VMEM((18, 8, WIDE), f32),
            pltpu.VMEM((2, 18, 8, 128), f32),
            pltpu.VMEM((8, 128), f32),
        ],
        compiler_params=pltpu.CompilerParams(vmem_limit_bytes=24 * 1024 * 1024),
    )(idx, *r, theta, flat)
    new_links = new_flat.reshape(3, 2, 3, 2, SLICES, SITES).transpose(4, 0, 1, 2, 3, 5)
    both = jnp.sum(lax.all_to_all(stats, SPACE, split_axis=0, concat_axis=0, tiled=True), axis=0)
    theta = both[8]
    deficit = both[:8]
    return (new_links, theta, deficit)


def solution(mesh):
    torus = Mesh(mesh.devices.reshape(4, 2, 8, 4), ("tm_0", "tm_1", "space_0", "space_1"))
    in_specs = (P(TM, None, None, None, None, SPACE),)
    out_specs = (P(TM, None, None, None, None, SPACE), P(), P(TM))
    return jax.shard_map(body, mesh=torus, in_specs=in_specs, out_specs=out_specs, check_vma=False)
```

```python
import functools
import math

import jax
import jax.numpy as jnp
import numpy as np
from jax import lax
from jax.experimental import pallas as pl
from jax.experimental.pallas import tpu as pltpu
from jax.sharding import Mesh
from jax.sharding import PartitionSpec as P

EXTENT = 48
SPACE = ("space_0", "space_1")
TM = ("tm_0", "tm_1")
TM_SPACE = ("tm_0", "tm_1", "space_0", "space_1")
SLICES = 8
ROWS = 72
SITES = ROWS * EXTENT
PLANE = EXTENT * EXTENT
WIDE = SITES + PLANE
WINDOW = WIDE + 128
BLOCK = 72
GROUP = 8 * PLANE

root_three = math.sqrt(3.0)
step_size = 0.08
f32 = jnp.float32
bf16 = jnp.bfloat16


def from_behind(block, axis, distance):
    n = lax.axis_size(axis)
    return lax.ppermute(block, axis, [((i - distance) % n, i) for i in range(n)])


def basis():
    k = np.arange(25)[:, None]
    x = np.arange(EXTENT)[None, :]
    cos = np.cos(2 * np.pi * k * x / EXTENT) * math.sqrt(2 / EXTENT)
    cos[0] /= math.sqrt(2)
    cos[24] /= math.sqrt(2)
    sin = np.sin(2 * np.pi * k * x / EXTENT) * math.sqrt(2 / EXTENT)
    return np.concatenate([cos, sin[1:24]], axis=0)


def wave_terms():
    k = np.concatenate([np.arange(25), np.arange(1, 24)])
    return 4 * np.sin(np.pi * k / EXTENT) ** 2


def split_bf16(a):
    a = np.asarray(a, np.float32)
    hi = a.astype(jnp.bfloat16)
    lo = (a - hi.astype(np.float32)).astype(jnp.bfloat16)
    return hi, lo


Q = basis()
P2 = wave_terms()
Q_HI, Q_LO = split_bf16(Q)
QT_HI, QT_LO = split_bf16(Q.T)
Q_STACK = np.concatenate([Q_HI, Q_HI, Q_LO], axis=1)
QT_STACK = np.concatenate([QT_HI, QT_HI, QT_LO], axis=1)
PZ = np.repeat(P2[:, None], 128, axis=1).astype(np.float32)
PX = P2.astype(np.float32)
PXM = np.repeat(np.repeat(P2.reshape(6, 1, 8), 6, axis=1).reshape(36, 8), 16, axis=1)
PZM = np.repeat(np.tile(P2.reshape(6, 8).T[:, None, :], (1, 6, 1)).reshape(8, 36, 1), 128, axis=2)
PSUM = (PXM[None] + PZM).astype(np.float32)


def zero_green(distance):
    d = np.arange(EXTENT)
    mean = np.mean(d * d / 96 - d / 2)
    return float(12 * (distance * distance / 96 - distance / 2 - mean))


def cmul(p, q):
    return (p[0] * q[0] - p[1] * q[1], p[0] * q[1] + p[1] * q[0])


def cmul_conj(p, q):
    return (p[0] * q[0] + p[1] * q[1], p[1] * q[0] - p[0] * q[1])


def cadd(p, q):
    return (p[0] + q[0], p[1] + q[1])


def csub(p, q):
    return (p[0] - q[0], p[1] - q[1])


def cross_conj(a, b):
    out = []
    for k in range(3):
        p = cmul(a[(k + 1) % 3], b[(k + 2) % 3])
        q = cmul(a[(k + 2) % 3], b[(k + 1) % 3])
        out.append((p[0] - q[0], q[1] - p[1]))
    return out


def algebra_of(u0, u1):
    u2 = cross_conj(u0, u1)
    return [
        u0[1][1] + u1[0][1],
        u0[1][0] - u1[0][0],
        u0[0][1] - u1[1][1],
        u0[2][1] + u2[0][1],
        u0[2][0] - u2[0][0],
        u1[2][1] + u2[1][1],
        u1[2][0] - u2[1][0],
        (u0[0][1] + u1[1][1] - 2.0 * u2[2][1]) * (1.0 / root_three),
    ]


def rotation_of(a):
    half = 0.5 * step_size
    a = [half * v for v in a]
    e = a[7] * (1.0 / root_three)
    diag = [a[2] + e, e - a[2], -2.0 * e]
    zero = jnp.zeros_like(a[0])
    x = [
        [(zero, diag[0]), (a[1], a[0]), (a[4], a[3])],
        [(-a[1], a[0]), (zero, diag[1]), (a[6], a[5])],
        [(-a[4], a[3]), (-a[6], a[5]), (zero, diag[2])],
    ]

    def entry(i, j):
        total = None
        for k in range(3):
            p, q = x[i][k], x[k][j]
            if i == k and k == j:
                term = (-p[1] * q[1], None)
            elif i == k:
                term = (-p[1] * q[1], p[1] * q[0])
            elif k == j:
                term = (-p[1] * q[1], p[0] * q[1])
            else:
                term = cmul(p, q)
            if total is None:
                total = term
            else:
                re = total[0] + term[0]
                if total[1] is None:
                    im = term[1]
                elif term[1] is None:
                    im = total[1]
                else:
                    im = total[1] + term[1]
                total = (re, im)
        re = 0.5 * total[0] + x[i][j][0] if i != j else 0.5 * total[0] + 1.0
        im = 0.5 * total[1] + x[i][j][1]
        return (re, im)

    m0 = [entry(0, j) for j in range(3)]
    m1 = [entry(1, j) for j in range(3)]
    inv = lax.rsqrt(sum(p[0] * p[0] + p[1] * p[1] for p in m0))
    r0 = [(p[0] * inv, p[1] * inv) for p in m0]
    corr = cmul_conj(m1[0], r0[0])
    for k in (1, 2):
        corr = cadd(corr, cmul_conj(m1[k], r0[k]))
    w = [csub(m1[k], cmul(corr, r0[k])) for k in range(3)]
    inv = lax.rsqrt(sum(p[0] * p[0] + p[1] * p[1] for p in w))
    r1 = [(p[0] * inv, p[1] * inv) for p in w]
    return r0, r1


def two_rows_of(load):
    u0 = [(load(2 * c), load(2 * c + 1)) for c in range(3)]
    u1 = [(load(6 + 2 * c), load(6 + 2 * c + 1)) for c in range(3)]
    return u0, u1


def project_kernel(links, hs):
    def project(q, carry):
        off = pl.multiple_of(q * 384, 128)
        for d in range(3):
            u0, u1 = two_rows_of(lambda n: links[12 * d + n, :, pl.ds(off, 384)])
            for c, h in enumerate(algebra_of(u0, u1)):
                hs[d * 8 + c, :, pl.ds(off, 384)] = h
        return carry

    lax.fori_loop(0, 9, project, 0)


def gradient_kernel(shift, idx, hs, out, zb):
    yc = idx[1]
    even = (yc % 2) == 0
    width = SITES + 128
    xzero = (lax.broadcasted_iota(jnp.int32, (8, SITES), 1) % EXTENT) == 0
    lane = lax.broadcasted_iota(jnp.int32, (8, 128), 1)
    first = lane < 48
    second = (lane >= 48) & (lane < 96)
    zeros = jnp.zeros((8, 128), f32)

    def combine(f, carry):
        c = 2 * lax.rem(yc + shift, 4) + f
        hx = hs[c]
        hy = jnp.concatenate([hs[8 + c], zeros], axis=1)
        hz = hs[16 + c]
        zb[...] = pltpu.roll(jnp.concatenate([hz, zeros], axis=1), 48, 1)
        head = zb[:, 0:128]
        zb[:, 0:128] = jnp.where(second & even, pltpu.roll(hz[:, 2304:2432], 48, 1), head)
        zb[:, 2304:2432] = jnp.where(second & even, 0.0, zb[:, 2304:2432])
        zb[:, 1152:1280] = jnp.where(second & jnp.logical_not(even), 0.0, zb[:, 1152:1280])
        bx = jnp.where(xzero, pltpu.roll(hx, SITES - 47, 1), pltpu.roll(hx, 1, 1))
        near = (bx - hx) - hz - hs[8 + c]
        p = jnp.concatenate([near, zeros], axis=1) + zb[...]
        p = pltpu.roll(p, 80, 1)
        ha = pltpu.roll(hy, 80, 1)
        out[f, :, 0:PLANE] = p[:, 0:PLANE]
        out[f, :, PLANE:width] = p[:, PLANE:width] + ha[:, 0 : width - PLANE]
        out[f, :, width:WINDOW] = ha[:, width - PLANE : width]
        wrap = jnp.where(even, hz[:, 0:128], hz[:, 1152:1280])
        out[f, :, WIDE:WINDOW] += pltpu.roll(jnp.where(first, wrap, 0.0), 80, 1)
        return carry

    for f in range(2):
        combine(f, 0)


def lambda_of(m):
    s = jnp.sqrt(m + 0.25 * m * m)
    return 1.0 / (1.0 + 0.5 * m + s), s


def split_value(a):
    hi = a.astype(bf16)
    return hi, (a - hi.astype(f32)).astype(bf16)


def dot(a, b, ca, cb):
    return lax.dot_general(a, b, (((ca,), (cb,)), ((), ())), preferred_element_type=f32)


def stack_of(a):
    hi, lo = split_value(a)
    return jnp.concatenate([hi, lo, hi], axis=0)


def decay_kernel(px, pz, after, lam_out, kap_out):
    def one(k, carry):
        lam, s = lambda_of(px[k] + pz[...])
        lam_out[k] = lam
        kap_out[k] = 6.0 / s
        return carry

    lax.fori_loop(0, EXTENT, one, 0)


def weight_kernel(px, pz, after, wa_out, wb_out):
    gi = lax.broadcasted_iota(jnp.int32, (EXTENT, 128), 1) // 16
    row = lax.broadcasted_iota(jnp.int32, (EXTENT, 128), 0)
    gr = 7 - gi

    def one(k, carry):
        lam, s = lambda_of(px[k] + pz[...])
        lam2 = lam * lam
        lam4 = lam2 * lam2
        wa = jnp.where(gi % 2 == 1, lam, 1.0) * jnp.where((gi // 2) % 2 == 1, lam2, 1.0)
        wa_out[k] = wa * jnp.where(gi >= 4, lam4, 1.0)
        wb = jnp.where(gr % 2 == 1, lam, 1.0) * jnp.where((gr // 2) % 2 == 1, lam2, 1.0)
        wb_out[k] = jnp.where((row == 0) & (k == 0), gi.astype(f32), wb * jnp.where(gr >= 4, lam4, 1.0))
        return carry

    lax.fori_loop(0, EXTENT, one, 0)


def matrix_kernel(qh, ql, qth, qtl, after, wxh, wxl, wxth, wxtl):
    def where_one(cond):
        return jnp.where(cond, 1.0, 0.0).astype(bf16)

    tall = lax.broadcasted_iota(jnp.int32, (384, EXTENT), 0)
    narrow = lax.broadcasted_iota(jnp.int32, (384, EXTENT), 1)
    wide = lax.broadcasted_iota(jnp.int32, (EXTENT, 384), 1)
    short = lax.broadcasted_iota(jnp.int32, (EXTENT, 384), 0)
    row = lax.broadcasted_iota(jnp.int32, (384, 384), 0)
    col = lax.broadcasted_iota(jnp.int32, (384, 384), 1)
    mask = (row % 8) == (col // EXTENT)
    mask_t = (row // EXTENT) == (col % 8)
    from_k = where_one(tall // 8 == narrow)
    to_x = where_one(wide % EXTENT == short)
    from_x = where_one(tall % EXTENT == narrow)
    to_k = where_one(wide // 8 == short)
    for q, out in ((qh, wxh), (ql, wxl)):
        a = dot(from_k, q[...], 1, 0).astype(bf16)
        out[...] = jnp.where(mask, dot(a, to_x, 1, 0), 0.0).astype(bf16)
    for q, out in ((qth, wxth), (qtl, wxtl)):
        a = dot(from_x, q[...], 1, 0).astype(bf16)
        out[...] = jnp.where(mask_t, dot(a, to_k, 1, 0), 0.0).astype(bf16)


def forward_kernel(
    idx, r0, r1, r2, r3, wxh, wxl, qs, lamt, kapt, m0, m1, m2, m3, m4, m5, m6, m7, own, e1o, e6o, theta, gs, ds, es, sout
):
    zc = idx[0]
    yc = idx[1]
    lane = lax.broadcasted_iota(jnp.int32, (8, 128), 1)
    gs[...] = jnp.zeros((2, 8, GROUP), f32)
    for k, r in enumerate((r0, r1, r2, r3)):
        yd = lax.rem(yc - k + 4, 4)
        off = pl.multiple_of(yd * SITES + PLANE - 128, 128)
        off_end = pl.multiple_of(yd * SITES + PLANE - 128 + WIDE, 128)
        off_wrap = pl.multiple_of(yd * SITES + lax.rem(yd, 2) * 1152, 128)
        for f in range(2):
            gs[f, :, pl.ds(off, WIDE)] += r[f, :, 0:WIDE]
            tail = r[f, :, WIDE:WINDOW]
            gs[f, :, pl.ds(off_end, 128)] += jnp.where(lane < 80, tail, 0.0)
            gs[f, :, pl.ds(off_wrap, 128)] += jnp.where(lane < 48, pltpu.roll(tail, 48, 1), 0.0)

    def along_x(j, carry):
        pieces = []
        for half in range(2):
            for n in range(8):
                for f in range(2):
                    place = PLANE * n + 384 * (2 * j + half)
                    pieces.append(gs[f, :, pl.ds(pl.multiple_of(place, 128), 384)])
        bh, bl = split_value(jnp.concatenate(pieces, axis=0))
        wh = wxh[...]
        out = dot(wh, bh, 1, 1) + dot(wh, bl, 1, 1) + dot(wxl[...], bh, 1, 1)
        for half in range(2):
            place = pl.multiple_of(8 * (2 * j + half), 8)
            ds[:, pl.ds(place, 8), :] = out[:, 128 * half : 128 * half + 128].reshape(EXTENT, 8, 128)
        return carry

    lax.fori_loop(0, 3, along_x, 0, unroll=True)

    gi = lax.broadcasted_iota(jnp.int32, (EXTENT, 128), 1) // 16

    def along_z(m, squares):
        packs = [jnp.zeros((EXTENT, 128), f32) for _ in range(6)]
        pair = None
        for g in range(8):
            k = m * 8 + g
            if g % 2 == 0:
                pair = dot(qs[...], stack_of(jnp.concatenate([ds[k], ds[k + 1]], axis=1)), 1, 0)
            e = pair[:, 128 * (g % 2) : 128 * (g % 2) + 128]
            if g == 0:
                es[m] = e[0:8]
            lam = lamt[k]
            lam2 = lam * lam
            lam4 = lam2 * lam2
            up = e + jnp.where(gi >= 1, lam, 0.0) * pltpu.roll(e, 16, 1)
            up = up + jnp.where(gi >= 2, lam2, 0.0) * pltpu.roll(up, 32, 1)
            up = up + jnp.where(gi >= 4, lam4, 0.0) * pltpu.roll(up, 64, 1)
            down = e + jnp.where(gi <= 6, lam, 0.0) * pltpu.roll(e, 112, 1)
            down = down + jnp.where(gi <= 5, lam2, 0.0) * pltpu.roll(down, 96, 1)
            down = down + jnp.where(gi <= 3, lam4, 0.0) * pltpu.roll(down, 64, 1)
            own[k] = kapt[k] * (up + down - e)
            squares = squares + sum(e[8 * i : 8 * i + 8] * e[8 * i : 8 * i + 8] for i in range(6))
            for n, (v, source) in enumerate(((up, 7), (down, 0), (e, 7), (e, 0), (e, 1), (e, 6))):
                shift = ((g - source) * 16) % 128
                packs[n] = jnp.where(gi == g, pltpu.roll(v, shift, 1) if shift else v, packs[n])
        for i in range(6):
            sout[pl.ds(m * 6 + i, 8, stride=72), :] = packs[0][8 * i : 8 * i + 8]
            sout[pl.ds(36 + m * 6 + i, 8, stride=72), :] = packs[1][8 * i : 8 * i + 8]
        m1[pl.ds(pl.multiple_of(BLOCK + 48 * m, 8), 48)] = packs[2]
        m7[pl.ds(pl.multiple_of(BLOCK + 48 * m, 8), 48)] = packs[3]
        e1o[m] = packs[4]
        e6o[m] = packs[5]
        return squares

    squares = lax.fori_loop(0, 6, along_z, jnp.zeros((8, 128), f32))

    e0 = es[0]
    gt = lane // 16
    row = lax.broadcasted_iota(jnp.int32, (8, 128), 0)
    total = zero_green(0) * e0
    for n in range(1, 8):
        weight = jnp.where(gt >= n, zero_green(n), zero_green(8 - n))
        total = total + weight * pltpu.roll(e0, 16 * n, 1)
    own[0, 0:8, :] = jnp.where(row == 0, total, own[0, 0:8, :])
    theta[...] = jnp.where((gt >= 2) & (gt <= 5), squares, 0.0)
    yf = gt.astype(f32)

    def over_groups(v):
        for n in (16, 32, 64):
            v = v + pltpu.roll(v, n, 1)
        return v

    first = over_groups(yf * e0)
    second = over_groups(yf * yf * e0)
    here = (row == 0) & (gt == 0)
    sout[0:8, :] = jnp.where(here, first, sout[0:8, :])
    sout[36:44, :] = jnp.where(here, second, sout[36:44, :])
    for k, o in enumerate((m0, m1, m2, m3, m4, m5, m6, m7)):
        o[0:BLOCK] = sout[pl.ds(pl.multiple_of(BLOCK * lax.rem(zc + k, 8), 8), BLOCK)]


def gather_z(zc, blocks, s):
    for k, r in enumerate(blocks):
        s[pl.ds(pl.multiple_of(BLOCK * lax.rem(zc - k + 8, 8), 8), BLOCK)] = r[0:BLOCK]


def solve_kernel(
    idx, r0, r1, r2, r3, r4, r5, r6, r7, psum, e1, e6, theta_in, o0, o1, o2, o3, o4, o5, o6, o7, theta, s, out
):
    zc = idx[0]
    gather_z(zc, (r0, r1, r2, r3, r4, r5, r6, r7), s)
    squares = theta_in[...]
    for m in range(6):
        for i in range(6):
            place = BLOCK + 48 * m + 8 * i
            plane_first = e1[m, 8 * i : 8 * i + 8] + r1[place : place + 8]
            plane_last = e6[m, 8 * i : 8 * i + 8] + r7[place : place + 8]
            squares = squares + plane_first * plane_first + plane_last * plane_last
    theta[...] = squares
    lam, root = lambda_of(psum[zc])
    lam2 = lam * lam
    lam6 = lam2 * lam2 * lam2
    lam12 = lam6 * lam6
    lam24 = lam12 * lam12
    row = lax.broadcasted_iota(jnp.int32, (36, 128), 0)
    lane = lax.broadcasted_iota(jnp.int32, (36, 128), 1)
    zero = (row == 0) & (lane < 16) & (zc == 0)
    kappa = 6.0 / root / (1.0 - lam24 * lam24)
    coef = []
    power = 1.0 + 0.5 * psum[zc] + root
    for k in range(1, 9):
        coef.append(kappa * power)
        power = power * lam6
    plus = [s[72 * n : 72 * n + 36, :] for n in range(8)]
    minus = [s[72 * n + 36 : 72 * n + 72, :] for n in range(8)]
    total_p = sum(plus)
    total_m = sum(minus)
    coef_a = [jnp.where(zero, 12.0 * (0.5 - k / 8.0) if k < 8 else 0.0, coef[k - 1]) for k in range(1, 9)]
    for t in range(8):
        a = coef_a[0] * plus[(t - 1) % 8]
        b = coef[0] * minus[(t + 1) % 8]
        for k in range(2, 9):
            a = a + coef_a[k - 1] * plus[(t - k) % 8]
            b = b + coef[k - 1] * minus[(t + k) % 8]
        a = a + jnp.where(zero, 0.125 * (total_m - minus[t]), 0.0)
        b = jnp.where(zero, -0.25 * (total_p - plus[t]), b)
        out[72 * t : 72 * t + 36, :] = a
        out[72 * t + 36 : 72 * t + 72, :] = b
    for k, o in enumerate((o0, o1, o2, o3, o4, o5, o6, o7)):
        o[...] = out[pl.ds(pl.multiple_of(BLOCK * lax.rem(zc + k, 8), 8), BLOCK)]


def spread_groups(v, gi):
    level = [v]
    for width in (4, 2, 1):
        bit = (gi // width) % 2
        out = []
        for a in level:
            if width == 4:
                rolled = pltpu.roll(a, 64, 1)
            else:
                up = pltpu.roll(a, 16 * width, 1)
                down = pltpu.roll(a, 128 - 16 * width, 1)
                rolled = jnp.where(bit == 0, down, up)
            out.append(jnp.where(bit == 0, a, rolled))
            out.append(jnp.where(bit == 0, rolled, a))
        level = out
    return level


def backward_kernel(
    idx, r0, r1, r2, r3, r4, r5, r6, r7, before, after, own, wxth, wxtl, qts, wat, wbt, o0, o1, o2, o3, ds, gs, ab
):
    yc = idx[1]
    gather_z(idx[0], (r0, r1, r2, r3, r4, r5, r6, r7), ab)
    gi = lax.broadcasted_iota(jnp.int32, (EXTENT, 128), 1) // 16

    def along_z(m, carry):
        ta = jnp.concatenate([ab[pl.ds(m * 6 + i, 8, stride=72), :] for i in range(6)], axis=0)
        tb = jnp.concatenate([ab[pl.ds(36 + m * 6 + i, 8, stride=72), :] for i in range(6)], axis=0)
        las = spread_groups(ta, gi)
        lbs = spread_groups(tb, gi)
        place = pl.multiple_of(BLOCK + 48 * m, 8)
        prior = -12.0 * before[pl.ds(place, 48)]
        later = -12.0 * after[pl.ds(place, 48)]
        u = []
        for g in range(8):
            k = m * 8 + g
            v = own[k] + las[g] * wat[k] + lbs[g] * wbt[k]
            shift = ((7 - g) * 16) % 128
            edge = jnp.where(gi == 0, pltpu.roll(prior, (-g * 16) % 128, 1) if g else prior, 0.0)
            edge = jnp.where(gi == 7, pltpu.roll(later, shift, 1) if shift else later, edge)
            u.append(v + edge)
            if g % 2 == 1:
                pair = dot(qts[...], stack_of(jnp.concatenate(u, axis=1)), 1, 0)
                ds[k - 1] = pair[:, 0:128]
                ds[k] = pair[:, 128:256]
                u = []
        return carry

    lax.fori_loop(0, 6, along_z, 0)

    def along_x(j, carry):
        halves = []
        for half in range(2):
            place = pl.multiple_of(8 * (2 * j + half), 8)
            halves.append(ds[:, pl.ds(place, 8), :].reshape(384, 128))
        dh, dl = split_value(jnp.concatenate(halves, axis=1))
        wh = wxth[...]
        o = dot(wh, dh, 1, 0) + dot(wh, dl, 1, 0) + dot(wxtl[...], dh, 1, 0)
        for half in range(2):
            t = jnp.transpose(o[:, 128 * half : 128 * half + 128])
            for n in range(8):
                for f in range(2):
                    place = PLANE * n + 384 * (2 * j + half)
                    gs[f, :, pl.ds(pl.multiple_of(place, 128), 384)] = t[16 * n + 8 * f : 16 * n + 8 * f + 8]
        return carry

    lax.fori_loop(0, 3, along_x, 0, unroll=True)
    for k, out in enumerate((o0, o1, o2, o3)):
        yd = lax.rem(yc + k, 4)
        off = pl.multiple_of(yd * SITES + PLANE - 128, 128)
        off_extra = pl.multiple_of(yd * SITES + lax.rem(yd, 2) * 1152, 128)
        for f in range(2):
            out[f, :, 0:WIDE] = pltpu.roll(gs[f, :, pl.ds(off, WINDOW)], WIDE + 48, 1)[:, 0:WIDE]
            out[f, :, WIDE:WINDOW] = gs[f, :, pl.ds(off_extra, 128)]


def rotate_kernel(idx, r0, r1, r2, r3, theta, links, out, stats, sm, ex, gs, fix, deficit):
    step = pl.program_id(0)
    yc = idx[1]
    even = (yc % 2) == 0
    lane = lax.broadcasted_iota(jnp.int32, (8, 128), 1)

    @pl.when(step == 0)
    def _():
        rotations_of((r0, r1, r2, r3), yc, sm, ex, gs, fix)
        deficit[...] = jnp.zeros((8, 128), f32)

    xlast = (lax.broadcasted_iota(jnp.int32, (8, 384), 1) % EXTENT) == EXTENT - 1

    def chunk(sub, carry):
        products(step * 3 + sub, sub, even, lane, xlast, links, out, gs, fix, deficit)
        return carry

    lax.fori_loop(0, 3, chunk, 0)

    @pl.when(step == 2)
    def _():
        row = lax.broadcasted_iota(jnp.int32, (8, 128), 0)
        line = jnp.sum(
            jnp.where(row == lane, jnp.sum(deficit[...], axis=1, keepdims=True), 0.0), axis=0, keepdims=True
        )
        total = jnp.sum(jnp.sum(theta[...], axis=1, keepdims=True), axis=0, keepdims=True)
        line = line * (1.0 / EXTENT**3)
        line = jnp.where(lane[0:1] == 8, total * (1.0 / (SLICES * 8 * EXTENT**3)), line)
        stats[...] = jnp.broadcast_to(line, (32, 128))


def rotations_of(received, yc, sm, ex, gs, fix):
    for k, r in enumerate(received):
        c0 = 2 * lax.rem(yc - k + 4, 4)
        for f in range(2):
            sm[c0 + f] = r[f, :, 0:WIDE]
            ex[c0 + f] = r[f, :, WIDE : WIDE + 128]

    def store_rotation(load, store):
        g0, g1 = rotation_of([load(c) for c in range(8)])
        g2 = cross_conj(g0, g1)
        for i, g in enumerate((g0, g1, g2)):
            for c in range(3):
                for p in range(2):
                    store(6 * i + 2 * c + p, g[c][p])

    def rotations(q, carry):
        off = pl.multiple_of(q * 384, 128)

        def store(n, v):
            gs[n, :, pl.ds(off, 384)] = v

        store_rotation(lambda c: sm[c, :, pl.ds(off, 384)], store)
        return carry

    lax.fori_loop(0, 15, rotations, 0)

    def store_fix(n, v):
        fix[0, n] = v

    store_rotation(lambda c: ex[c], store_fix)
    for n in range(18):
        fix[1, n] = pltpu.roll(gs[n, :, 0:128], 80, 1)


def products(q, sub, even, lane, xlast, links, out, gs, fix, deficit):
    local = pl.multiple_of(sub * 384, 128)
    off = pl.multiple_of(q * 384, 128)
    far = pl.multiple_of(q * 384 + PLANE, 128)
    from_fix = ((q == 0) & even) | ((q == 3) & jnp.logical_not(even)) | ((q == 6) & even)
    which = jnp.where(q == 6, 1, 0)
    head = (lane < 48) & from_fix

    def here(n):
        return gs[n, :, pl.ds(off, 384)]

    def ahead_x(n):
        v = here(n)
        return jnp.where(xlast, pltpu.roll(v, 47, 1), pltpu.roll(v, 383, 1))

    def ahead_y(n):
        return gs[n, :, pl.ds(far, 384)]

    def ahead_z(n):
        v = pltpu.roll(gs[n, :, pl.ds(off, 512)], 512 - 48, 1)[:, 0:384]
        return jnp.concatenate([jnp.where(head, fix[which, n], v[:, 0:128]), v[:, 128:384]], axis=1)

    def matrix(load):
        return [[(load(6 * i + 2 * c), load(6 * i + 2 * c + 1)) for c in range(3)] for i in range(3)]

    g = matrix(here)
    acc = jnp.zeros((8, 384), f32)
    for d, ahead in enumerate((ahead_x, ahead_y, ahead_z)):
        u0, u1 = two_rows_of(lambda n: links[12 * d + n, :, pl.ds(off, 384)])
        u = [u0, u1, cross_conj(u0, u1)]
        h = matrix(ahead)
        rows_out = []
        for i in range(2):
            t = []
            for j in range(3):
                v = cmul(g[i][0], u[0][j])
                for k in (1, 2):
                    v = cadd(v, cmul(g[i][k], u[k][j]))
                t.append(v)
            line = []
            for j in range(3):
                v = cmul_conj(t[0], h[j][0])
                for k in (1, 2):
                    v = cadd(v, cmul_conj(t[k], h[j][k]))
                line.append(v)
                out[12 * d + 6 * i + 2 * j, :, pl.ds(local, 384)] = v[0]
                out[12 * d + 6 * i + 2 * j + 1, :, pl.ds(local, 384)] = v[1]
            rows_out.append(line)
        a, b = rows_out
        corner = (a[0][0] * b[1][0] - a[0][1] * b[1][1]) - (a[1][0] * b[0][0] - a[1][1] * b[0][1])
        acc = acc + (3.0 - a[0][0] - b[1][0] - corner)
    deficit[...] += acc[:, 0:128] + acc[:, 128:256] + acc[:, 256:384]


def shape(*dims):
    return jax.ShapeDtypeStruct(dims, f32)


def call(kernel, outs, scalars, scratch=()):
    def run(*args):
        vm = pl.BlockSpec(memory_space=pltpu.VMEM)
        sm = pl.BlockSpec(memory_space=pltpu.SMEM)
        return pl.pallas_call(
            kernel,
            in_specs=[sm] * scalars + [vm] * (len(args) - scalars),
            out_specs=[vm] * len(outs),
            out_shape=list(outs),
            scratch_shapes=list(scratch),
            compiler_params=pltpu.CompilerParams(vmem_limit_bytes=24 * 1024 * 1024),
        )(*args)

    return run


def exchange_y(pieces):
    return [pieces[0]] + [from_behind(pieces[k], "space_1", k) for k in (1, 2, 3)]


def exchange_z(blocks):
    return [blocks[0]] + [from_behind(blocks[k], "space_0", k) for k in range(1, 8)]


def body(links):
    zc = lax.axis_index("space_0")
    yc = lax.axis_index("space_1")
    idx = jnp.stack([zc, yc]).astype(jnp.int32)
    px = jnp.asarray(PX)
    flat = links.transpose(1, 2, 3, 4, 0, 5).reshape(36, SLICES, SITES)
    window = shape(2, 8, WINDOW)
    modes = shape(48, 48, 128)
    packed = shape(6, 48, 128)
    (hs,) = call(project_kernel, [shape(24, 8, SITES)], 0)(flat)
    pieces = []
    for k in range(4):
        piece = functools.partial(gradient_kernel, k)
        (piece,) = call(piece, [window], 1, [pltpu.VMEM((8, SITES + 128), f32)])(idx, hs)
        pieces.append(piece)
    r = exchange_y(pieces)
    lam, kap = call(decay_kernel, [modes] * 2, 1)(px, jnp.asarray(PZ), hs)
    square = jax.ShapeDtypeStruct((384, 384), bf16)
    wxh, wxl, wxth, wxtl = call(matrix_kernel, [square] * 4, 0)(
        jnp.asarray(Q_HI), jnp.asarray(Q_LO), jnp.asarray(QT_HI), jnp.asarray(QT_LO), hs
    )
    block = shape(BLOCK, 128)
    long_block = shape(BLOCK + 288, 128)
    *blocks, own, e1, e6, theta = call(
        forward_kernel,
        [block, long_block] + [block] * 5 + [long_block, modes, packed, packed, shape(8, 128)],
        1,
        [
            pltpu.VMEM((2, 8, GROUP), f32),
            pltpu.VMEM((48, 48, 128), f32),
            pltpu.VMEM((6, 8, 128), f32),
            pltpu.VMEM((576, 128), f32),
        ],
    )(idx, *r, wxh, wxl, jnp.asarray(Q_STACK), lam, kap)
    blocks = exchange_z(blocks)
    before, after = blocks[1], blocks[7]
    *amps, theta = call(
        solve_kernel, [block] * 8 + [shape(8, 128)], 1, [pltpu.VMEM((576, 128), f32)] * 2
    )(idx, *blocks, jnp.asarray(PSUM), e1, e6, theta)
    wa, wb = call(weight_kernel, [modes] * 2, 1)(px, jnp.asarray(PZ), amps[0])
    theta = theta + from_behind(theta, "tm_1", 1)
    theta = theta + sum(from_behind(theta, "tm_0", k) for k in (1, 2, 3))
    amps = exchange_z(amps)
    windows = call(
        backward_kernel,
        [window] * 4,
        1,
        [pltpu.VMEM((48, 48, 128), f32), pltpu.VMEM((2, 8, GROUP), f32), pltpu.VMEM((576, 128), f32)],
    )(
        idx, *amps, before, after, own, wxth, wxtl, jnp.asarray(QT_STACK), wa, wb,
    )
    r = exchange_y(windows)
    again, _ = lax.optimization_barrier((links, windows[1]))
    flat = again.transpose(1, 2, 3, 4, 0, 5).reshape(36, SLICES, SITES)
    vm = pl.BlockSpec(memory_space=pltpu.VMEM)
    new_flat, stats = pl.pallas_call(
        rotate_kernel,
        grid=(3,),
        in_specs=[pl.BlockSpec(memory_space=pltpu.SMEM)] + [vm] * 6,
        out_specs=[pl.BlockSpec((36, 8, 1152), lambda q: (0, 0, q)), pl.BlockSpec((32, 128), lambda q: (0, 0))],
        out_shape=[pltpu.HBM((36, 8, SITES), f32), shape(32, 128)],
        scratch_shapes=[
            pltpu.VMEM((8, 8, WIDE), f32),
            pltpu.VMEM((8, 8, 128), f32),
            pltpu.VMEM((18, 8, WIDE), f32),
            pltpu.VMEM((2, 18, 8, 128), f32),
            pltpu.VMEM((8, 128), f32),
        ],
        compiler_params=pltpu.CompilerParams(vmem_limit_bytes=24 * 1024 * 1024),
    )(idx, *r, theta, flat)
    new_links = new_flat.reshape(3, 2, 3, 2, SLICES, SITES).transpose(4, 0, 1, 2, 3, 5)
    both = jnp.sum(lax.all_to_all(stats, SPACE, split_axis=0, concat_axis=0, tiled=True), axis=0)
    theta = both[8]
    deficit = both[:8]
    return (new_links, theta, deficit)


def solution(mesh):
    torus = Mesh(mesh.devices.reshape(4, 2, 8, 4), ("tm_0", "tm_1", "space_0", "space_1"))
    in_specs = (P(TM, None, None, None, None, SPACE),)
    out_specs = (P(TM, None, None, None, None, SPACE), P(), P(TM))
    return jax.shard_map(body, mesh=torus, in_specs=in_specs, out_specs=out_specs, check_vma=False)
```
